8 devices in a mesh: rhs: 1 (over z), col: 2 (over y), row: 4 (over x, core).
Axes of the slice: x: 2, y: 2, z: 1, core: 2. Of those that a mesh axis runs over, the one named last changes fastest.
Arguments:
- volume: bfloat16 [128, 128, 128, 64], P('row', 'col', None, 'rhs')
- a_one: bfloat16 [128, 128], replicated
- b_one: bfloat16 [128, 128], replicated
- a_two: bfloat16 [128, 128], replicated
- b_two: bfloat16 [128, 128], replicated
- a_three: bfloat16 [128, 128], replicated
- b_three: bfloat16 [128, 128], replicated
- spectrum: float32 [128, 128, 128], P('row', 'col')
Outputs:
- output: float32 [128, 128, 128, 64], P('row', 'col', None, 'rhs')
All inputs are finite; a program needn't handle non-finite values.
Results may differ from the reference program's by a relative error of at most 0.0126449.
Values are sent between devices in bfloat16 or wider.
A program may use at most 1 GiB of HBM per device.

```python
import jax
import jax.numpy as jnp

N1 = 128
N2 = 128
N3 = 128
C = 64


def orthonormal(rng_key, order_n):
    q_mat = jnp.linalg.qr(jax.random.normal(rng_key, (order_n, order_n), jnp.float32))[0]
    return q_mat.astype(jnp.bfloat16)


def setup_inputs(seed: int = 0, part: int = 0) -> dict:
    shared = jax.random.split(jax.random.key(seed), 7)
    vol_key = jax.random.fold_in(jax.random.key(seed + 1), part)
    volume = jax.random.normal(vol_key, (N1, N2, N3, C), jnp.float32).astype(jnp.bfloat16)
    spectrum = jnp.exp(jax.random.uniform(shared[6], (N1, N2, N3), jnp.float32, -1.15, 1.15))
    return {'volume': volume, 'a_one': orthonormal(shared[0], N1), 'b_one': orthonormal(shared[1], N1), 'a_two': orthonormal(shared[2], N2), 'b_two': orthonormal(shared[3], N2), 'a_three': orthonormal(shared[4], N3), 'b_three': orthonormal(shared[5], N3), 'spectrum': spectrum}


def mode_product(factor, tensor, form):
    return jnp.einsum(form, factor.astype(jnp.float32), tensor.astype(jnp.float32))


def reference(volume, a_one, b_one, a_two, b_two, a_three, b_three, spectrum):
    u_three = mode_product(a_three, volume, 'ka,ijar->ijkr').astype(jnp.bfloat16)
    u_one = mode_product(a_one, u_three, 'ia,ajkr->ijkr').astype(jnp.bfloat16)
    u_two = mode_product(a_two, u_one, 'ja,iakr->ijkr').astype(jnp.bfloat16)
    scaled = (spectrum[:, :, :, None] * u_two.astype(jnp.float32)).astype(jnp.bfloat16)
    v_two = mode_product(b_two, scaled, 'ja,iakr->ijkr').astype(jnp.bfloat16)
    v_one = mode_product(b_one, v_two, 'ia,ajkr->ijkr').astype(jnp.bfloat16)
    return mode_product(b_three, v_one, 'ka,ijar->ijkr')
```

```python
import functools

import jax
import jax.numpy as jnp
from jax import lax
from jax.experimental import pallas as pl
from jax.experimental.pallas import tpu as pltpu
from jax.sharding import PartitionSpec as P

F32 = jnp.float32
BF16 = jnp.bfloat16
MESH = pl.DeviceIdType.MESH
ND = 8
JB = 4
PA = 72
PB = 136
JC = 2


def dot(a, b):
    return jnp.dot(a, b, preferred_element_type=F32)


def exchange_kernel(x, w3, a1, a2, b2, b1, d, u3, recv, vs, q,
                    xb, ub, ta, p, u1, v2, vo, tb, dv,
                    xsem, usem, psem, vsem, dsem, dss, drs, oss, ors, rss, rrs):
    row, col = lax.axis_index('row'), lax.axis_index('col')
    me = col * 4 + row

    def peer(s):
        return {'row': row ^ (s & 3), 'col': col ^ (s >> 2)}

    def idx(s):
        return (col ^ (s >> 2)) * 4 + (row ^ (s & 3))

    def rows_of(s):
        return pl.ds(pl.multiple_of((row ^ (s & 3)) * 32, 32), 32)

    def cols_of(s):
        return pl.ds(pl.multiple_of((col ^ (s >> 2)) * 64, 64), 64)

    def remote(src, dst, send, recv_, s):
        return pltpu.make_async_remote_copy(
            src_ref=src, dst_ref=dst, send_sem=send, recv_sem=recv_,
            device_id=peer(s), device_id_type=MESH)

    bar = pltpu.get_barrier_semaphore()
    for s in range(1, ND):
        pl.semaphore_signal(bar, inc=1, device_id=peer(s), device_id_type=MESH)
    pl.semaphore_wait(bar, ND - 1)

    own_d = pltpu.make_async_copy(d, dv.at[rows_of(0), cols_of(0), :], dsem)
    own_d.start()

    def d_out(s):
        return remote(d, dv.at[rows_of(0), cols_of(0), :], dss.at[s], drs.at[s], s)

    def d_in(s):
        return remote(d, dv.at[rows_of(s), cols_of(s), :], dss.at[s], drs.at[s], s)

    for s in (2, 4, 6):
        d_out(s).start()

    def x_load(c, t, slot):
        return pltpu.make_async_copy(
            x.at[:, pl.ds(t * JB, JB), pl.ds(pl.multiple_of(c * 16, 16), 16), :],
            xb.at[slot], xsem.at[slot])

    def u_store(c, t, slot):
        return pltpu.make_async_copy(
            ub.at[slot], u3.at[c, :, pl.ds(t * JB, JB), :, :], usem.at[slot])

    def out_copy(ch, s):
        return remote(u3.at[ch // 2, (ch % 2) * 8 + idx(s)], recv.at[ch, me],
                      oss.at[ch, s], ors.at[ch, s], s)

    def out_arrival(ch, s):
        return remote(u3.at[ch // 2, (ch % 2) * 8 + idx(s)], recv.at[ch, idx(s)],
                      oss.at[ch, s], ors.at[ch, s], s)

    nt = 64 // JB

    def group(c, carry):
        x_load(c, 0, 0).start()

        def block(t, carry):
            slot = lax.rem(t, 2)

            @pl.when(t + 1 < nt)
            def _():
                x_load(c, t + 1, 1 - slot).start()

            x_load(c, t, slot).wait()

            @pl.when(t >= 2)
            def _():
                u_store(c, t - 2, slot).wait()

            lo = xb[slot, 0:16].reshape(16 * JB * 16, 128)
            hi = xb[slot, 16:32].reshape(16 * JB * 16, 128)
            y = dot(jnp.concatenate([lo, hi], axis=1), w3[...])
            n = JB * 16
            for i in range(16):
                ta[i * PA:i * PA + n, :] = y[i * n:(i + 1) * n, :128]
                ta[(i + 16) * PA:(i + 16) * PA + n, :] = y[i * n:(i + 1) * n, 128:]

            for r in range(16):
                for j in range(JB):
                    ub[slot, r, j] = ta[pl.ds(j * 16 + r, 32, stride=PA), :].astype(BF16)
            u_store(c, t, slot).start()
            return carry

        lax.fori_loop(0, nt, block, 0)
        u_store(c, nt - 2, (nt - 2) % 2).wait()
        u_store(c, nt - 1, (nt - 1) % 2).wait()
        for h in range(2):
            for s in range(1, ND):
                out_copy(2 * c + h, s).start()
        return carry

    lax.fori_loop(0, 4, group, 0)

    own_d.wait()
    for s in (2, 4, 6):
        d_in(s).wait_recv()

    def d_relay(s):
        return remote(dv.at[rows_of(s), cols_of(s), :], dv.at[rows_of(s), cols_of(s), :],
                      dss.at[s + 1], drs.at[s + 1], 1)

    def d_relayed(s):
        return remote(dv.at[rows_of(s), cols_of(s), :], dv.at[rows_of(s + 1), cols_of(s + 1), :],
                      dss.at[s + 1], drs.at[s + 1], 1)

    for s in (0, 2, 4, 6):
        d_relay(s).start()
    for s in (0, 2, 4, 6):
        d_relayed(s).wait_recv()

    def back_copy(ch, s):
        return remote(vs.at[ch, s], q.at[ch, me], rss.at[ch, s], rrs.at[ch, s], s)

    def back_arrival(ch, s):
        return remote(vs.at[ch, s], q.at[ch, idx(s)], rss.at[ch, s], rrs.at[ch, s], s)

    def swap_out(dst, g):
        def body(i, carry):
            for e in range(16):
                n = i * 16 + e
                dst[n, pl.ds(pl.multiple_of(g * 16, 16), 16), :] = (
                    tb[pl.ds(n, 16, stride=PB), :].astype(BF16))
            return carry
        lax.fori_loop(0, 8, body, 0)

    def chunk(ch, carry):
        for s in range(1, ND):
            out_arrival(ch, s).wait_recv()
        loads = []
        for s in range(ND):
            src = recv.at[ch, idx(s)] if s else u3.at[ch // 2, (ch % 2) * 8 + me]
            loads.append(pltpu.make_async_copy(
                src, p.at[cols_of(s), rows_of(s), :], psem.at[s]))
            loads[-1].start()
        for load in loads:
            load.wait()

        def one(g, carry):
            for e in range(8):
                j = g * 16 + 2 * e
                y = dot(a1[...], jnp.concatenate([p[j], p[j + 1]], axis=1))
                tb[2 * e * PB:2 * e * PB + 128, :] = y[:, :128]
                tb[(2 * e + 1) * PB:(2 * e + 1) * PB + 128, :] = y[:, 128:]
            swap_out(u1, g)
            return carry

        lax.fori_loop(0, 8, one, 0)

        def two(g, carry):
            for e in range(8):
                i = g * 16 + 2 * e
                y = dot(a2[...], jnp.concatenate([u1[i], u1[i + 1]], axis=1))
                y = y.astype(BF16).astype(F32)
                w = jnp.concatenate([dv[i], dv[i + 1]], axis=1) * y
                z = dot(b2[...], w.astype(BF16))
                tb[2 * e * PB:2 * e * PB + 128, :] = z[:, :128]
                tb[(2 * e + 1) * PB:(2 * e + 1) * PB + 128, :] = z[:, 128:]
            swap_out(v2, g)
            return carry

        lax.fori_loop(0, 8, two, 0)

        def three(g, carry):
            for e in range(4):
                j = g * 8 + 2 * e
                y = dot(b1[...], jnp.concatenate([v2[j], v2[j + 1]], axis=1)).astype(BF16)
                vo[j] = y[:, :128]
                vo[j + 1] = y[:, 128:]
            return carry

        lax.fori_loop(0, 16, three, 0)

        stores = []
        for s in range(ND):
            dst = vs.at[ch, s] if s else q.at[ch, me]
            stores.append(pltpu.make_async_copy(
                vo.at[cols_of(s), rows_of(s), :], dst, vsem.at[s]))
            stores[-1].start()
        for store in stores:
            store.wait()
        for s in range(1, ND):
            back_copy(ch, s).start()
        return carry

    lax.fori_loop(0, ND, chunk, 0)

    for s in (2, 4, 6):
        d_out(s).wait_send()
    for s in (0, 2, 4, 6):
        d_relay(s).wait_send()

    def finish(ch, carry):
        for s in range(1, ND):
            out_copy(ch, s).wait_send()
            back_copy(ch, s).wait_send()
            back_arrival(ch, s).wait_recv()
        return carry

    lax.fori_loop(0, ND, finish, 0)


def exchange(x, w3, a1, a2, b2, b1, d):
    hbm = pl.BlockSpec(memory_space=pl.ANY)
    vmem = pl.BlockSpec(memory_space=pltpu.VMEM)
    dma = pltpu.SemaphoreType.DMA
    piece = (64, 32, 128)
    return pl.pallas_call(
        exchange_kernel,
        out_shape=[
            jax.ShapeDtypeStruct((4, 16) + piece, BF16),
            jax.ShapeDtypeStruct((ND, ND) + piece, BF16),
            jax.ShapeDtypeStruct((ND, ND) + piece, BF16),
            jax.ShapeDtypeStruct((ND, ND) + piece, BF16),
        ],
        in_specs=[hbm, vmem, vmem, vmem, vmem, vmem, hbm],
        out_specs=[hbm] * 4,
        scratch_shapes=[
            pltpu.VMEM((2, 32, JB, 16, 128), BF16),
            pltpu.VMEM((2, 16, JB, 32, 128), BF16),
            pltpu.VMEM((32 * PA, 128), F32),
            pltpu.VMEM((128, 128, 128), BF16),
            pltpu.VMEM((128, 128, 128), BF16),
            pltpu.VMEM((128, 128, 128), BF16),
            pltpu.VMEM((128, 128, 128), BF16),
            pltpu.VMEM((16 * PB, 128), F32),
            pltpu.VMEM((128, 128, 128), F32),
            dma((2,)), dma((2,)), dma((ND,)), dma((ND,)), dma(()),
            dma((ND,)), dma((ND,)),
            dma((ND, ND)), dma((ND, ND)), dma((ND, ND)), dma((ND, ND)),
        ],
        compiler_params=pltpu.CompilerParams(
            collective_id=0, has_side_effects=True, vmem_limit_bytes=56 * 1024 * 1024),
        name='exchange',
    )(x, w3, a1, a2, b2, b1, d)[3]


PC = JC * 32 + 8


def last_kernel(q, b3t, z, t):
    n = JC * 32
    y = dot(q[...].reshape(64 * n, 128), b3t[...])
    for r in range(64):
        t[r * PC:r * PC + n, :] = y[r * n:(r + 1) * n]

    for j in range(JC):
        for i in range(32):
            z[i, j] = t[pl.ds(j * 32 + i, 64, stride=PC), :]


def last(q, b3t):
    return pl.pallas_call(
        last_kernel,
        grid=(64 // JC,),
        out_shape=jax.ShapeDtypeStruct((32, 64, 64, 128), F32),
        in_specs=[
            pl.BlockSpec((64, JC, 32, 128), lambda j: (0, j, 0, 0)),
            pl.BlockSpec((128, 128), lambda j: (0, 0)),
        ],
        out_specs=pl.BlockSpec((32, JC, 64, 128), lambda j: (0, j, 0, 0)),
        scratch_shapes=[pltpu.VMEM((64 * PC, 128), F32)],
        compiler_params=pltpu.CompilerParams(vmem_limit_bytes=40 * 1024 * 1024),
        name='last',
    )(q, b3t)


def solution(mesh):
    vol_spec = P('row', 'col', None, 'rhs')
    diag_spec = P('row', 'col', None)
    full_spec = P(None, None)

    def local_op(volume, a_one, b_one, a_two, b_two, a_three, b_three, spectrum):
        x = jnp.transpose(volume, (0, 1, 3, 2))
        a3t = a_three.T
        zero = jnp.zeros_like(a3t)
        w3 = jnp.concatenate([jnp.concatenate([a3t, zero], 1), jnp.concatenate([zero, a3t], 1)], 0)
        q = exchange(x, w3, a_one, a_two, b_two, b_one, spectrum)
        z = last(q.reshape(64, 64, 32, 128), b_three.T)
        return jnp.transpose(z, (0, 1, 3, 2))

    return jax.shard_map(
        local_op, mesh=mesh,
        in_specs=(vol_spec, full_spec, full_spec, full_spec, full_spec, full_spec, full_spec, diag_spec),
        out_specs=vol_spec, check_vma=False)
```

```python
import functools

import jax
import jax.numpy as jnp
from jax import lax
from jax.experimental import pallas as pl
from jax.experimental.pallas import tpu as pltpu
from jax.sharding import PartitionSpec as P

F32 = jnp.float32
BF16 = jnp.bfloat16
MESH = pl.DeviceIdType.MESH
ND = 8
JB = 4
PA = 72
PB = 136
NE = ND - 1
JC = 2
JF = 8


def dot(a, b):
    return jnp.dot(a, b, preferred_element_type=F32)


def exchange_kernel(x, w3, a1, a2, b2, b1, d, u3, recv, vs, q,
                    f0, f1, f2, f3, f4, f5, f6, f7, xb, ub, ta, p, u1, v2, vo, tb, dv,
                    xsem, usem, psem, vsem, dsem, dss, drs, oss, ors, rss, rrs):
    row, col = lax.axis_index('row'), lax.axis_index('col')
    me = col * 4 + row

    def peer(s):
        return {'row': row ^ (s & 3), 'col': col ^ (s >> 2)}

    def idx(s):
        return (col ^ (s >> 2)) * 4 + (row ^ (s & 3))

    def rows_of(s):
        return pl.ds(pl.multiple_of((row ^ (s & 3)) * 32, 32), 32)

    def cols_of(s):
        return pl.ds(pl.multiple_of((col ^ (s >> 2)) * 64, 64), 64)

    def remote(src, dst, send, recv_, s):
        return pltpu.make_async_remote_copy(
            src_ref=src, dst_ref=dst, send_sem=send, recv_sem=recv_,
            device_id=peer(s), device_id_type=MESH)

    bar = pltpu.get_barrier_semaphore()
    for s in range(1, ND):
        pl.semaphore_signal(bar, inc=1, device_id=peer(s), device_id_type=MESH)
    pl.semaphore_wait(bar, ND - 1)

    own_d = pltpu.make_async_copy(d, dv.at[rows_of(0), cols_of(0), :], dsem)
    own_d.start()

    def d_out(s):
        return remote(d, dv.at[rows_of(0), cols_of(0), :], dss.at[s], drs.at[s], s)

    def d_in(s):
        return remote(d, dv.at[rows_of(s), cols_of(s), :], dss.at[s], drs.at[s], s)

    for s in (2, 4, 6):
        d_out(s).start()

    def x_load(c, t, slot):
        return pltpu.make_async_copy(
            x.at[:, pl.ds(t * JB, JB), pl.ds(pl.multiple_of(c * 16, 16), 16), :],
            xb.at[slot], xsem.at[slot])

    def u_store(c, t, slot):
        return pltpu.make_async_copy(
            ub.at[slot], u3.at[c, :, pl.ds(t * JB, JB), :, :], usem.at[slot])

    def out_copy(ch, s):
        return remote(u3.at[ch // 2, (ch % 2) * 8 + idx(s)], recv.at[ch, me],
                      oss.at[ch, s], ors.at[ch, s], s)

    def out_arrival(ch, s):
        return remote(u3.at[ch // 2, (ch % 2) * 8 + idx(s)], recv.at[ch, idx(s)],
                      oss.at[ch, s], ors.at[ch, s], s)

    nt = 64 // JB

    def group(c, carry):
        x_load(c, 0, 0).start()

        def block(t, carry):
            slot = lax.rem(t, 2)

            @pl.when(t + 1 < nt)
            def _():
                x_load(c, t + 1, 1 - slot).start()

            x_load(c, t, slot).wait()

            @pl.when(t >= 2)
            def _():
                u_store(c, t - 2, slot).wait()

            lo = xb[slot, 0:16].reshape(16 * JB * 16, 128)
            hi = xb[slot, 16:32].reshape(16 * JB * 16, 128)
            y = dot(jnp.concatenate([lo, hi], axis=1), w3[...])
            n = JB * 16
            for i in range(16):
                ta[i * PA:i * PA + n, :] = y[i * n:(i + 1) * n, :128]
                ta[(i + 16) * PA:(i + 16) * PA + n, :] = y[i * n:(i + 1) * n, 128:]

            for r in range(16):
                for j in range(JB):
                    ub[slot, r, j] = ta[pl.ds(j * 16 + r, 32, stride=PA), :].astype(BF16)
            u_store(c, t, slot).start()
            return carry

        lax.fori_loop(0, nt, block, 0)
        u_store(c, nt - 2, (nt - 2) % 2).wait()
        u_store(c, nt - 1, (nt - 1) % 2).wait()
        for h in range(2):
            for s in range(1, ND):
                out_copy(2 * c + h, s).start()
        return carry

    lax.fori_loop(0, 4, group, 0)

    own_d.wait()
    for s in (2, 4, 6):
        d_in(s).wait_recv()

    def d_relay(s):
        return remote(dv.at[rows_of(s), cols_of(s), :], dv.at[rows_of(s), cols_of(s), :],
                      dss.at[s + 1], drs.at[s + 1], 1)

    def d_relayed(s):
        return remote(dv.at[rows_of(s), cols_of(s), :], dv.at[rows_of(s + 1), cols_of(s + 1), :],
                      dss.at[s + 1], drs.at[s + 1], 1)

    for s in (0, 2, 4, 6):
        d_relay(s).start()
    for s in (0, 2, 4, 6):
        d_relayed(s).wait_recv()

    def back_copy(ch, s):
        return remote(vs.at[ch, s], q.at[ch, me], rss.at[ch, s], rrs.at[ch, s], s)

    def back_arrival(ch, s):
        return remote(vs.at[ch, s], q.at[ch, idx(s)], rss.at[ch, s], rrs.at[ch, s], s)

    def swap_out(dst, g):
        def body(i, carry):
            for e in range(16):
                n = i * 16 + e
                dst[n, pl.ds(pl.multiple_of(g * 16, 16), 16), :] = (
                    tb[pl.ds(n, 16, stride=PB), :].astype(BF16))
            return carry
        lax.fori_loop(0, 8, body, 0)

    def chunk(ch, final):
        for s in range(1, ND):
            out_arrival(ch, s).wait_recv()
        loads = []
        for s in range(ND):
            src = recv.at[ch, idx(s)] if s else u3.at[ch // 2, (ch % 2) * 8 + me]
            loads.append(pltpu.make_async_copy(
                src, p.at[cols_of(s), rows_of(s), :], psem.at[s]))
            loads[-1].start()
        for load in loads:
            load.wait()

        def one(g, carry):
            for e in range(8):
                j = g * 16 + 2 * e
                y = dot(a1[...], jnp.concatenate([p[j], p[j + 1]], axis=1))
                tb[2 * e * PB:2 * e * PB + 128, :] = y[:, :128]
                tb[(2 * e + 1) * PB:(2 * e + 1) * PB + 128, :] = y[:, 128:]
            swap_out(u1, g)
            return carry

        lax.fori_loop(0, 8, one, 0)

        def two(g, carry):
            for e in range(8):
                i = g * 16 + 2 * e
                y = dot(a2[...], jnp.concatenate([u1[i], u1[i + 1]], axis=1))
                y = y.astype(BF16).astype(F32)
                w = jnp.concatenate([dv[i], dv[i + 1]], axis=1) * y
                z = dot(b2[...], w.astype(BF16))
                tb[2 * e * PB:2 * e * PB + 128, :] = z[:, :128]
                tb[(2 * e + 1) * PB:(2 * e + 1) * PB + 128, :] = z[:, 128:]
            swap_out(v2, g)
            return carry

        lax.fori_loop(0, 8, two, 0)

        def three(g, carry):
            for e in range(4):
                j = g * 8 + 2 * e
                y = dot(b1[...], jnp.concatenate([v2[j], v2[j + 1]], axis=1)).astype(BF16)
                vo[j] = y[:, :128]
                vo[j + 1] = y[:, 128:]
            return carry

        lax.fori_loop(0, 16, three, 0)

        stores = []
        for s in range(ND):
            dst = final[s] if final else vs.at[ch, s] if s else q.at[ch, me]
            stores.append(pltpu.make_async_copy(
                vo.at[cols_of(s), rows_of(s), :], dst, vsem.at[s]))
            stores[-1].start()
        for store in stores:
            store.wait()
        if not final:
            for s in range(1, ND):
                back_copy(ch, s).start()

    def early(ch, carry):
        chunk(ch, None)
        return carry

    lax.fori_loop(0, NE, early, 0)
    chunk(NE, (f0, f1, f2, f3, f4, f5, f6, f7))

    for s in (2, 4, 6):
        d_out(s).wait_send()
    for s in (0, 2, 4, 6):
        d_relay(s).wait_send()

    def finish(ch, carry):
        for s in range(1, ND):
            out_copy(ch, s).wait_send()
            back_copy(ch, s).wait_send()
            back_arrival(ch, s).wait_recv()
        return carry

    lax.fori_loop(0, NE, finish, 0)
    for s in range(1, ND):
        out_copy(NE, s).wait_send()


def exchange(x, w3, a1, a2, b2, b1, d):
    hbm = pl.BlockSpec(memory_space=pl.ANY)
    vmem = pl.BlockSpec(memory_space=pltpu.VMEM)
    dma = pltpu.SemaphoreType.DMA
    piece = (64, 32, 128)
    return pl.pallas_call(
        exchange_kernel,
        out_shape=[
            jax.ShapeDtypeStruct((4, 16) + piece, BF16),
            jax.ShapeDtypeStruct((ND, ND) + piece, BF16),
            jax.ShapeDtypeStruct((NE, ND) + piece, BF16),
            jax.ShapeDtypeStruct((NE, ND) + piece, BF16),
        ] + [jax.ShapeDtypeStruct(piece, BF16)] * ND,
        in_specs=[hbm, vmem, vmem, vmem, vmem, vmem, hbm],
        out_specs=[hbm] * (4 + ND),
        scratch_shapes=[
            pltpu.VMEM((2, 32, JB, 16, 128), BF16),
            pltpu.VMEM((2, 16, JB, 32, 128), BF16),
            pltpu.VMEM((32 * PA, 128), F32),
            pltpu.VMEM((128, 128, 128), BF16),
            pltpu.VMEM((128, 128, 128), BF16),
            pltpu.VMEM((128, 128, 128), BF16),
            pltpu.VMEM((128, 128, 128), BF16),
            pltpu.VMEM((16 * PB, 128), F32),
            pltpu.VMEM((128, 128, 128), F32),
            dma((2,)), dma((2,)), dma((ND,)), dma((ND,)), dma(()),
            dma((ND,)), dma((ND,)),
            dma((ND, ND)), dma((ND, ND)), dma((NE, ND)), dma((NE, ND)),
        ],
        compiler_params=pltpu.CompilerParams(
            collective_id=0, has_side_effects=True, vmem_limit_bytes=56 * 1024 * 1024),
        name='exchange',
    )(x, w3, a1, a2, b2, b1, d)[3:]


PC = JC * 32 + 8
PF = JF * 32 + 8


def early_kernel(q, b3t, z, t):
    n = JC * 32
    y = dot(q[...].reshape(NE * ND * n, 128), b3t[...])
    for r in range(NE * ND):
        t[r * PC:r * PC + n, :] = y[r * n:(r + 1) * n]

    for j in range(JC):
        for i in range(32):
            z[i, j] = t[pl.ds(j * 32 + i, NE * ND, stride=PC), :]


def early_last(q, b3t):
    nr = NE * ND
    return pl.pallas_call(
        early_kernel,
        grid=(64 // JC,),
        out_shape=jax.ShapeDtypeStruct((32, 64, 64, 128), F32),
        in_specs=[
            pl.BlockSpec((nr, JC, 32, 128), lambda j: (0, j, 0, 0)),
            pl.BlockSpec((128, 128), lambda j: (0, 0)),
        ],
        out_specs=pl.BlockSpec((32, JC, nr, 128), lambda j: (0, j, 0, 0)),
        scratch_shapes=[pltpu.VMEM((nr * PC, 128), F32)],
        compiler_params=pltpu.CompilerParams(vmem_limit_bytes=40 * 1024 * 1024),
        cost_estimate=pl.CostEstimate(
            flops=2 * nr * 64 * 32 * 128 * 128, bytes_accessed=nr * 64 * 32 * 128 * 6, transcendentals=0),
        name='early_last',
    )(q, b3t)


def final_kernel(f0, f1, f2, f3, f4, f5, f6, f7, b3t, z_in, z, t):
    row, col = lax.axis_index('row'), lax.axis_index('col')
    n = JF * 32
    for s, f in enumerate((f0, f1, f2, f3, f4, f5, f6, f7)):
        r = (col ^ (s >> 2)) * 4 + (row ^ (s & 3))
        y = dot(f[...].reshape(n, 128), b3t[...])
        t[pl.ds(pl.multiple_of(r * PF, 8), n), :] = y

    for j in range(JF):
        for i in range(32):
            z[i, j] = t[pl.ds(j * 32 + i, ND, stride=PF), :]


def final_last(pieces, b3t, z):
    return pl.pallas_call(
        final_kernel,
        grid=(64 // JF,),
        out_shape=jax.ShapeDtypeStruct((32, 64, 64, 128), F32),
        in_specs=[pl.BlockSpec((JF, 32, 128), lambda j: (j, 0, 0))] * ND + [
            pl.BlockSpec((128, 128), lambda j: (0, 0)),
            pl.BlockSpec(memory_space=pl.ANY),
        ],
        out_specs=pl.BlockSpec((32, JF, ND, 128), lambda j: (0, j, NE, 0)),
        scratch_shapes=[pltpu.VMEM((ND * PF, 128), F32)],
        input_output_aliases={ND + 1: 0},
        compiler_params=pltpu.CompilerParams(vmem_limit_bytes=40 * 1024 * 1024),
        cost_estimate=pl.CostEstimate(
            flops=2 * ND * 64 * 32 * 128 * 128, bytes_accessed=ND * 64 * 32 * 128 * 6, transcendentals=0),
        name='final_last',
    )(*pieces, b3t, z)


def solution(mesh):
    vol_spec = P('row', 'col', None, 'rhs')
    diag_spec = P('row', 'col', None)
    full_spec = P(None, None)

    def local_op(volume, a_one, b_one, a_two, b_two, a_three, b_three, spectrum):
        x = jnp.transpose(volume, (0, 1, 3, 2))
        a3t = a_three.T
        zero = jnp.zeros_like(a3t)
        w3 = jnp.concatenate([jnp.concatenate([a3t, zero], 1), jnp.concatenate([zero, a3t], 1)], 0)
        b3t = b_three.T
        q, *pieces = exchange(x, w3, a_one, a_two, b_two, b_one, spectrum)
        pieces[1:] = [
            lax.ppermute(pieces[s], ('col', 'row'), [(m, m ^ s) for m in range(ND)])
            for s in range(1, ND)]
        z = early_last(q.reshape(NE * ND, 64, 32, 128), b3t)
        z = final_last(pieces, b3t, z)
        return jnp.transpose(z, (0, 1, 3, 2))

    return jax.shard_map(
        local_op, mesh=mesh,
        in_specs=(vol_spec, full_spec, full_spec, full_spec, full_spec, full_spec, full_spec, diag_spec),
        out_specs=vol_spec, check_vma=False)
```

```python
import jax
import jax.numpy as jnp
from jax import lax
from jax.experimental import pallas as pl
from jax.experimental.pallas import tpu as pltpu
from jax.sharding import PartitionSpec as P

F32 = jnp.float32
BF16 = jnp.bfloat16
MESH = pl.DeviceIdType.MESH
ND = 8
NE = ND - 1
JB = 4
PA = JB * 16 + 8
PB = 136
JC = 2
JF = 8


def dot(a, b):
    return jnp.dot(a, b, preferred_element_type=F32)


def exchange_kernel(x, a3, a1, a2, b2, b1, b3, d, u3, recv, vs, q,
                    f0, f1, f2, f3, f4, f5, f6, f7, wb,
                    xb, ub, ta, xs, w3, wv, p, u1, v2, vo, tb, dl, dp, dr, dv,
                    xsem, usem, psem, vsem, dsem, wsem, dss, drs, oss, ors, rss, rrs):
    row, col = lax.axis_index('row'), lax.axis_index('col')
    me = col * 4 + row

    def peer(s):
        return {'row': row ^ (s & 3), 'col': col ^ (s >> 2)}

    def idx(s):
        return (col ^ (s >> 2)) * 4 + (row ^ (s & 3))

    def chip(s):
        return lax.div(idx(s), 2)

    def core(s):
        return lax.rem(row ^ (s & 3), 2)

    def rows_of(s):
        return pl.ds(pl.multiple_of((row ^ (s & 3)) * 32, 32), 32)

    def cols_of(s):
        return pl.ds(pl.multiple_of((col ^ (s >> 2)) * 64, 64), 64)

    def remote(src, dst, send, recv_, s):
        return pltpu.make_async_remote_copy(
            src_ref=src, dst_ref=dst, send_sem=send, recv_sem=recv_,
            device_id=peer(s), device_id_type=MESH)

    own_d = pltpu.make_async_copy(d, dl, dsem)
    own_d.start()

    bar = pltpu.get_barrier_semaphore()
    for s in range(1, ND):
        pl.semaphore_signal(bar, inc=1, device_id=peer(s), device_id_type=MESH)

    lane = lax.broadcasted_iota(jnp.int32, (16, 128), 1)
    own_d.wait()

    def pack(i, carry):
        parts = [dl[i, 16 * b:16 * b + 16, :] for b in range(4)]
        for c in range(4):
            out = parts[0] if c == 0 else pltpu.roll(parts[0], (128 - 32 * c) % 128, 1)
            for b in range(1, 4):
                sh = (32 * (b - c)) % 128
                v = pltpu.roll(parts[b], sh, 1) if sh else parts[b]
                out = jnp.where(lane >= 32 * b, v, out)
            dp[c, i] = out
        return carry

    lax.fori_loop(0, 32, pack, 0)

    w3[...] = jnp.zeros_like(w3)
    for c in range(4):
        for r in range(4):
            w3[c * 128 + r * 32:c * 128 + r * 32 + 32, r * 128:r * 128 + 128] = (
                a3[c * 32:c * 32 + 32, :])

    pl.semaphore_wait(bar, ND - 1)

    def d_out(s):
        return remote(dp.at[chip(s)], dr.at[me], dss.at[s], drs.at[s], s)

    def d_in(s):
        return remote(dp.at[chip(s)], dr.at[idx(s)], dss.at[s], drs.at[s], s)

    for s in (2, 4, 6):
        d_out(s).start()

    def x_load(c, t, slot):
        return pltpu.make_async_copy(
            x.at[:, pl.ds(t * JB, JB), pl.ds(pl.multiple_of(c * 16, 16), 16), :],
            xb.at[slot], xsem.at[slot])

    def u_store(c, t, slot):
        return pltpu.make_async_copy(
            ub.at[slot], u3.at[c, :, :, pl.ds(t * JB, JB), :, :], usem.at[slot])

    def out_src(ch, s):
        return u3.at[ch // 2, (ch % 2) * 2 + core(s), chip(s)]

    def out_copy(ch, s):
        return remote(out_src(ch, s), recv.at[ch, me], oss.at[ch, s], ors.at[ch, s], s)

    def out_arrival(ch, s):
        return remote(out_src(ch, s), recv.at[ch, idx(s)], oss.at[ch, s], ors.at[ch, s], s)

    nt = 64 // JB

    def group(c, carry):
        x_load(c, 0, 0).start()

        def block(t, carry):
            slot = lax.rem(t, 2)

            @pl.when(t + 1 < nt)
            def _():
                x_load(c, t + 1, 1 - slot).start()

            x_load(c, t, slot).wait()

            @pl.when(t >= 2)
            def _():
                u_store(c, t - 2, slot).wait()

            n = JB * 16
            for i in range(32):
                ta[i * PA:i * PA + n, :] = xb[slot, i].reshape(n, 128).astype(F32)
            m = JB * 32
            for r in range(16):
                for j in range(JB):
                    xs[(r // 4) * m + j * 32:(r // 4) * m + j * 32 + 32, (r % 4) * 128:(r % 4) * 128 + 128] = (
                        ta[pl.ds(j * 16 + r, 32, stride=PA), :].astype(BF16))
            y = lax.dot_general(xs[...], w3[...], (((1,), (1,)), ((), ())),
                                preferred_element_type=F32).astype(BF16)
            for g in range(4):
                for c4 in range(4):
                    ub[slot, g, c4] = y[g * m:(g + 1) * m, c4 * 128:c4 * 128 + 128].reshape(JB, 32, 128)
            u_store(c, t, slot).start()
            return carry

        lax.fori_loop(0, nt, block, 0)
        u_store(c, nt - 2, (nt - 2) % 2).wait()
        u_store(c, nt - 1, (nt - 1) % 2).wait()
        for h in range(2):
            for s in range(1, ND):
                out_copy(2 * c + h, s).start()
        return carry

    lax.fori_loop(0, 4, group, 0)

    wv[...] = jnp.zeros_like(wv)
    b3t = b3[...].astype(F32).T.astype(BF16)
    for c in range(4):
        for r in range(4):
            wv[c * 128 + r * 32:c * 128 + r * 32 + 32, r * 128:r * 128 + 128] = (
                b3t[c * 32:c * 32 + 32, :])
    w_store = pltpu.make_async_copy(wv, wb, wsem)
    w_store.start()

    for s in (2, 4, 6):
        d_in(s).wait_recv()

    def d_src(s):
        return dr.at[idx(s)] if s else dp.at[chip(0)]

    def d_relay(s):
        return remote(d_src(s), dr.at[idx(s)], dss.at[s + 1], drs.at[s + 1], 1)

    def d_relayed(s):
        return remote(d_src(s), dr.at[idx(s + 1)], dss.at[s + 1], drs.at[s + 1], 1)

    for s in (0, 2, 4, 6):
        d_relay(s).start()
    for s in (0, 2, 4, 6):
        d_relayed(s).wait_recv()

    def unpack(i, carry):
        for s in range(ND):
            g = dr[idx(s), i] if s else dp[chip(0), i]
            base_i = (row ^ (s & 3)) * 32
            base_j = (col ^ (s >> 2)) * 64
            for b in range(4):
                pair = pltpu.roll(g, 32 if b % 2 == 0 else 96, 1)
                v = jnp.where(lax.div(lane, 32) == b, g, pair)
                v = jnp.where(lax.div(lane, 64) == b // 2, v, pltpu.roll(v, 64, 1))
                dv[base_i + i, pl.ds(pl.multiple_of(base_j + 16 * b, 16), 16), :] = v
        return carry

    lax.fori_loop(0, 32, unpack, 0)

    def back_copy(ch, s):
        return remote(vs.at[ch, s], q.at[ch, me], rss.at[ch, s], rrs.at[ch, s], s)

    def back_arrival(ch, s):
        return remote(vs.at[ch, s], q.at[ch, idx(s)], rss.at[ch, s], rrs.at[ch, s], s)

    def swap_out(dst, g):
        def body(i, carry):
            for e in range(16):
                n = i * 16 + e
                dst[n, pl.ds(pl.multiple_of(g * 16, 16), 16), :] = (
                    tb[pl.ds(n, 16, stride=PB), :].astype(BF16))
            return carry
        lax.fori_loop(0, 8, body, 0)

    def chunk(ch, final):
        for s in range(1, ND):
            out_arrival(ch, s).wait_recv()
        loads = []
        for s in range(ND):
            src = recv.at[ch, idx(s)] if s else out_src(ch, 0)
            loads.append(pltpu.make_async_copy(
                src, p.at[cols_of(s), rows_of(s), :], psem.at[s]))
            loads[-1].start()
        for load in loads:
            load.wait()

        def one(g, carry):
            for e in range(8):
                j = g * 16 + 2 * e
                y = dot(a1[...], jnp.concatenate([p[j], p[j + 1]], axis=1))
                tb[2 * e * PB:2 * e * PB + 128, :] = y[:, :128]
                tb[(2 * e + 1) * PB:(2 * e + 1) * PB + 128, :] = y[:, 128:]
            swap_out(u1, g)
            return carry

        lax.fori_loop(0, 8, one, 0)

        def two(g, carry):
            for e in range(8):
                i = g * 16 + 2 * e
                y = dot(a2[...], jnp.concatenate([u1[i], u1[i + 1]], axis=1))
                y = y.astype(BF16).astype(F32)
                w = jnp.concatenate([dv[i], dv[i + 1]], axis=1) * y
                z = dot(b2[...], w.astype(BF16))
                tb[2 * e * PB:2 * e * PB + 128, :] = z[:, :128]
                tb[(2 * e + 1) * PB:(2 * e + 1) * PB + 128, :] = z[:, 128:]
            swap_out(v2, g)
            return carry

        lax.fori_loop(0, 8, two, 0)

        def three(g, carry):
            for e in range(4):
                j = g * 8 + 2 * e
                y = dot(b1[...], jnp.concatenate([v2[j], v2[j + 1]], axis=1)).astype(BF16)
                vo[j] = y[:, :128]
                vo[j + 1] = y[:, 128:]
            return carry

        lax.fori_loop(0, 16, three, 0)

        stores = []
        for s in range(ND):
            dst = final[s] if final else vs.at[ch, s] if s else q.at[ch, me]
            stores.append(pltpu.make_async_copy(
                vo.at[cols_of(s), rows_of(s), :], dst, vsem.at[s]))
            stores[-1].start()
        for store in stores:
            store.wait()
        if not final:
            for s in range(1, ND):
                back_copy(ch, s).start()

    def early(ch, carry):
        chunk(ch, None)
        return carry

    lax.fori_loop(0, NE, early, 0)
    chunk(NE, (f0, f1, f2, f3, f4, f5, f6, f7))

    w_store.wait()
    for s in (2, 4, 6):
        d_out(s).wait_send()
    for s in (0, 2, 4, 6):
        d_relay(s).wait_send()

    def finish(ch, carry):
        for s in range(1, ND):
            out_copy(ch, s).wait_send()
            back_copy(ch, s).wait_send()
            back_arrival(ch, s).wait_recv()
        return carry

    lax.fori_loop(0, NE, finish, 0)
    for s in range(1, ND):
        out_copy(NE, s).wait_send()


def exchange(x, a3, a1, a2, b2, b1, b3, d):
    hbm = pl.BlockSpec(memory_space=pl.ANY)
    vmem = pl.BlockSpec(memory_space=pltpu.VMEM)
    dma = pltpu.SemaphoreType.DMA
    piece = (64, 32, 128)
    return pl.pallas_call(
        exchange_kernel,
        out_shape=[
            jax.ShapeDtypeStruct((4, 4, 4) + piece, BF16),
            jax.ShapeDtypeStruct((ND, ND) + piece, BF16),
            jax.ShapeDtypeStruct((NE, ND) + piece, BF16),
            jax.ShapeDtypeStruct((NE, ND) + piece, BF16),
        ] + [jax.ShapeDtypeStruct(piece, BF16)] * ND + [
            jax.ShapeDtypeStruct((512, 512), BF16),
        ],
        in_specs=[hbm] + [vmem] * 6 + [hbm],
        out_specs=[hbm] * (5 + ND),
        scratch_shapes=[
            pltpu.VMEM((2, 32, JB, 16, 128), BF16),
            pltpu.VMEM((2, 4, 4, JB, 32, 128), BF16),
            pltpu.VMEM((32 * PA, 128), F32),
            pltpu.VMEM((JB * 128, 512), BF16),
            pltpu.VMEM((512, 512), BF16),
            pltpu.VMEM((512, 512), BF16),
            pltpu.VMEM((128, 128, 128), BF16),
            pltpu.VMEM((128, 128, 128), BF16),
            pltpu.VMEM((128, 128, 128), BF16),
            pltpu.VMEM((128, 128, 128), BF16),
            pltpu.VMEM((16 * PB, 128), F32),
            pltpu.VMEM((32, 64, 128), F32),
            pltpu.VMEM((4, 32, 16, 128), F32),
            pltpu.VMEM((ND, 32, 16, 128), F32),
            pltpu.VMEM((128, 128, 128), F32),
            dma((2,)), dma((2,)), dma((ND,)), dma((ND,)), dma(()), dma(()),
            dma((ND,)), dma((ND,)),
            dma((ND, ND)), dma((ND, ND)), dma((NE, ND)), dma((NE, ND)),
        ],
        compiler_params=pltpu.CompilerParams(
            collective_id=0, has_side_effects=True, vmem_limit_bytes=56 * 1024 * 1024),
        name='exchange',
    )(x, a3, a1, a2, b2, b1, b3, d)[3:]


PC = JC * 32 + 8
PF = JF * 32 + 8


def early_kernel(q, wb, z, t):
    n = JC * 32
    parts = [q[:, c].reshape(NE * 2 * n, 128) for c in range(4)]
    y = dot(jnp.concatenate(parts, axis=1), wb[...])
    for g in range(NE * 2):
        for r in range(4):
            k = (4 * g + r) * PC
            t[k:k + n, :] = y[g * n:(g + 1) * n, r * 128:r * 128 + 128]

    for j in range(JC):
        for i in range(32):
            z[i, j] = t[pl.ds(j * 32 + i, NE * ND, stride=PC), :]


def early_last(q, wb):
    nr = NE * ND
    return pl.pallas_call(
        early_kernel,
        grid=(64 // JC,),
        out_shape=jax.ShapeDtypeStruct((32, 64, 64, 128), F32),
        in_specs=[
            pl.BlockSpec((NE, 4, 2, JC, 32, 128), lambda j: (0, 0, 0, j, 0, 0)),
            pl.BlockSpec((512, 512), lambda j: (0, 0)),
        ],
        out_specs=pl.BlockSpec((32, JC, nr, 128), lambda j: (0, j, 0, 0)),
        scratch_shapes=[pltpu.VMEM((nr * PC, 128), F32)],
        compiler_params=pltpu.CompilerParams(vmem_limit_bytes=40 * 1024 * 1024),
        cost_estimate=pl.CostEstimate(
            flops=2 * nr * 64 * 32 * 128 * 128, bytes_accessed=nr * 64 * 32 * 128 * 6, transcendentals=0),
        name='early_last',
    )(q.reshape(NE, 4, 2, 64, 32, 128), wb)


def final_kernel(f0, f1, f2, f3, f4, f5, f6, f7, wb, z_in, z, t):
    f = (f0, f1, f2, f3, f4, f5, f6, f7)
    row, col = lax.axis_index('row'), lax.axis_index('col')
    chip, core = col * 2 + lax.div(row, 2), lax.rem(row, 2)
    n = JF * 32
    w = jnp.concatenate(
        [wb[pl.ds(pl.multiple_of((chip ^ c) * 128, 128), 128), :] for c in range(4)], axis=0)
    for h in range(2):
        parts = [f[2 * c + h][...].reshape(n, 128) for c in range(4)]
        y = dot(jnp.concatenate(parts, axis=1), w)
        for r in range(4):
            k = ((core ^ h) * 4 + r) * PF
            t[pl.ds(pl.multiple_of(k, 8), n), :] = y[:, r * 128:r * 128 + 128]

    for j in range(JF):
        for i in range(32):
            z[i, j] = t[pl.ds(j * 32 + i, ND, stride=PF), :]


def final_last(pieces, wb, z):
    return pl.pallas_call(
        final_kernel,
        grid=(64 // JF,),
        out_shape=jax.ShapeDtypeStruct((32, 64, 64, 128), F32),
        in_specs=[pl.BlockSpec((JF, 32, 128), lambda j: (j, 0, 0))] * ND + [
            pl.BlockSpec((512, 512), lambda j: (0, 0)),
            pl.BlockSpec(memory_space=pl.ANY),
        ],
        out_specs=pl.BlockSpec((32, JF, ND, 128), lambda j: (0, j, NE, 0)),
        scratch_shapes=[pltpu.VMEM((ND * PF, 128), F32)],
        input_output_aliases={ND + 1: 0},
        compiler_params=pltpu.CompilerParams(vmem_limit_bytes=40 * 1024 * 1024),
        cost_estimate=pl.CostEstimate(
            flops=2 * ND * 64 * 32 * 128 * 128, bytes_accessed=ND * 64 * 32 * 128 * 6, transcendentals=0),
        name='final_last',
    )(*pieces, wb, z)


def solution(mesh):
    vol_spec = P('row', 'col', None, 'rhs')
    diag_spec = P('row', 'col', None)
    full_spec = P(None, None)

    def local_op(volume, a_one, b_one, a_two, b_two, a_three, b_three, spectrum):
        x = jnp.transpose(volume, (0, 1, 3, 2))
        q, *pieces, wb = exchange(x, a_three, a_one, a_two, b_two, b_one, b_three, spectrum)
        pieces[1:] = [
            lax.ppermute(pieces[s], ('col', 'row'), [(m, m ^ s) for m in range(ND)])
            for s in range(1, ND)]
        z = early_last(q, wb)
        z = final_last(pieces, wb, z)
        return jnp.transpose(z, (0, 1, 3, 2))

    return jax.shard_map(
        local_op, mesh=mesh,
        in_specs=(vol_spec, full_spec, full_spec, full_spec, full_spec, full_spec, full_spec, diag_spec),
        out_specs=vol_spec, check_vma=False)
```

```python
import jax
import jax.numpy as jnp
from jax import lax
from jax.experimental import pallas as pl
from jax.experimental.pallas import tpu as pltpu
from jax.sharding import PartitionSpec as P

F32 = jnp.float32
BF16 = jnp.bfloat16
MESH = pl.DeviceIdType.MESH
ND = 8
ORDER = (6, 4, 2, 7, 5, 3, 1)
NE = ND - 1
JB = 4
PA = JB * 16 + 8
PB = 136
JC = 4
JA = 48
JF = 8


def dot(a, b):
    return jnp.dot(a, b, preferred_element_type=F32)


def exchange_kernel(x, a3_in, a1_in, a2_in, b2_in, b1_in, b3_in, d, u3, recv, vs, q,
                    ga0, ga1, ga2, ga3, gb0, gb1, gb2, gb3, wb,
                    a3, a1, a2, b2, b1, b3, xb, ub, ta, xs, w3, wv, p, u1, v2, vo, tb, dl, dp, dr, dv,
                    xsem, usem, psem, vsem, dsem, wsem, fsem, dss, drs, oss, ors, rss, rrs, gss, grs):
    row, col = lax.axis_index('row'), lax.axis_index('col')
    me = col * 4 + row

    def peer(s):
        return {'row': row ^ (s & 3), 'col': col ^ (s >> 2)}

    def idx(s):
        return (col ^ (s >> 2)) * 4 + (row ^ (s & 3))

    def chip(s):
        return lax.div(idx(s), 2)

    def core(s):
        return lax.rem(row ^ (s & 3), 2)

    def rows_of(s):
        return pl.ds(pl.multiple_of((row ^ (s & 3)) * 32, 32), 32)

    def cols_of(s):
        return pl.ds(pl.multiple_of((col ^ (s >> 2)) * 64, 64), 64)

    def remote(src, dst, send, recv_, s):
        return pltpu.make_async_remote_copy(
            src_ref=src, dst_ref=dst, send_sem=send, recv_sem=recv_,
            device_id=peer(s), device_id_type=MESH)

    bar = pltpu.get_barrier_semaphore()
    for s in range(1, ND):
        pl.semaphore_signal(bar, inc=1, device_id=peer(s), device_id_type=MESH)

    own_d = pltpu.make_async_copy(d, dl, dsem)
    own_d.start()
    factors = [pltpu.make_async_copy(src, dst, fsem.at[n]) for n, (src, dst) in enumerate(
        ((a3_in, a3), (a1_in, a1), (a2_in, a2), (b2_in, b2), (b1_in, b1), (b3_in, b3)))]
    for factor in factors:
        factor.start()

    lane = lax.broadcasted_iota(jnp.int32, (16, 128), 1)
    own_d.wait()

    def pack(i, carry):
        parts = [dl[i, 16 * b:16 * b + 16, :] for b in range(4)]
        for c in range(4):
            out = parts[0] if c == 0 else pltpu.roll(parts[0], (128 - 32 * c) % 128, 1)
            for b in range(1, 4):
                sh = (32 * (b - c)) % 128
                v = pltpu.roll(parts[b], sh, 1) if sh else parts[b]
                out = jnp.where(lane >= 32 * b, v, out)
            dp[c, i] = out
        return carry

    lax.fori_loop(0, 32, pack, 0, unroll=4)

    pl.semaphore_wait(bar, ND - 1)

    def d_out(s):
        return remote(dp.at[chip(s)], dr.at[me], dss.at[s], drs.at[s], s)

    def d_in(s):
        return remote(dp.at[chip(s)], dr.at[idx(s)], dss.at[s], drs.at[s], s)

    for s in (6, 4, 2):
        d_out(s).start()

    for factor in factors:
        factor.wait()

    w3[...] = jnp.zeros_like(w3)
    for c in range(4):
        for r in range(4):
            w3[c * 128 + r * 32:c * 128 + r * 32 + 32, r * 128:r * 128 + 128] = (
                a3[c * 32:c * 32 + 32, :])

    def x_load(c, t, slot):
        return pltpu.make_async_copy(
            x.at[:, pl.ds(t * JB, JB), pl.ds(pl.multiple_of(c * 16, 16), 16), :],
            xb.at[slot], xsem.at[slot])

    def u_store(c, t, slot):
        return pltpu.make_async_copy(
            ub.at[slot], u3.at[c, :, :, pl.ds(t * JB, JB), :, :], usem.at[slot])

    def out_src(ch, s):
        return u3.at[ch // 2, (ch % 2) * 2 + core(s), chip(s)]

    def out_copy(ch, s):
        return remote(out_src(ch, s), recv.at[ch, me], oss.at[ch, s], ors.at[ch, s], s)

    def out_slab(ch, s, b):
        part = pl.ds(b * 16, 16)
        return remote(out_src(ch, s).at[part], recv.at[ch, me].at[part],
                      oss.at[ch, s], ors.at[ch, s], s)

    def send_slab(c, b):
        for h in range(2):
            for s in ORDER:
                out_slab(2 * c + h, s, b).start()

    def out_arrival(ch, s):
        return remote(out_src(ch, s), recv.at[ch, idx(s)], oss.at[ch, s], ors.at[ch, s], s)

    nt = 64 // JB

    def group(c, carry):
        x_load(c, 0, 0).start()

        def block(t, carry):
            slot = lax.rem(t, 2)

            @pl.when(t + 1 < nt)
            def _():
                x_load(c, t + 1, 1 - slot).start()

            x_load(c, t, slot).wait()

            @pl.when(t >= 2)
            def _():
                u_store(c, t - 2, slot).wait()

            @pl.when(jnp.logical_and(lax.rem(t, 4) == 1, t > 4))
            def _():
                send_slab(c, lax.div(t, 4) - 1)

            n = JB * 16
            for i in range(32):
                ta[i * PA:i * PA + n, :] = xb[slot, i].reshape(n, 128).astype(F32)
            m = JB * 32
            for r in range(16):
                for j in range(JB):
                    xs[(r // 4) * m + j * 32:(r // 4) * m + j * 32 + 32, (r % 4) * 128:(r % 4) * 128 + 128] = (
                        ta[pl.ds(j * 16 + r, 32, stride=PA), :].astype(BF16))
            y = lax.dot_general(xs[...], w3[...], (((1,), (1,)), ((), ())),
                                preferred_element_type=F32).astype(BF16)
            for g in range(4):
                for c4 in range(4):
                    ub[slot, g, c4] = y[g * m:(g + 1) * m, c4 * 128:c4 * 128 + 128].reshape(JB, 32, 128)
            u_store(c, t, slot).start()
            return carry

        lax.fori_loop(0, nt, block, 0)
        u_store(c, nt - 2, (nt - 2) % 2).wait()
        u_store(c, nt - 1, (nt - 1) % 2).wait()
        send_slab(c, 3)
        return carry

    lax.fori_loop(0, 4, group, 0)

    wv[...] = jnp.zeros_like(wv)
    b3t = b3[...].astype(F32).T.astype(BF16)
    for c in range(4):
        for r in range(4):
            wv[c * 128 + r * 32:c * 128 + r * 32 + 32, r * 128:r * 128 + 128] = (
                b3t[c * 32:c * 32 + 32, :])
    w_store = pltpu.make_async_copy(wv, wb, wsem)
    w_store.start()

    for s in (2, 4, 6):
        d_in(s).wait_recv()

    def d_src(s):
        return dr.at[idx(s)] if s else dp.at[chip(0)]

    def d_relay(s):
        return remote(d_src(s), dr.at[idx(s)], dss.at[s + 1], drs.at[s + 1], 1)

    def d_relayed(s):
        return remote(d_src(s), dr.at[idx(s + 1)], dss.at[s + 1], drs.at[s + 1], 1)

    for s in (0, 2, 4, 6):
        d_relay(s).start()
    for s in (0, 2, 4, 6):
        d_relayed(s).wait_recv()

    def unpack(i, carry):
        for s in range(ND):
            g = dr[idx(s), i] if s else dp[chip(0), i]
            base_i = (row ^ (s & 3)) * 32
            base_j = (col ^ (s >> 2)) * 64
            for b in range(4):
                pair = pltpu.roll(g, 32 if b % 2 == 0 else 96, 1)
                v = jnp.where(lax.div(lane, 32) == b, g, pair)
                v = jnp.where(lax.div(lane, 64) == b // 2, v, pltpu.roll(v, 64, 1))
                dv[base_i + i, pl.ds(pl.multiple_of(base_j + 16 * b, 16), 16), :] = v
        return carry

    lax.fori_loop(0, 32, unpack, 0)

    def back_copy(ch, s):
        return remote(vs.at[ch, s], q.at[ch, me], rss.at[ch, s], rrs.at[ch, s], s)

    def back_arrival(ch, s):
        return remote(vs.at[ch, s], q.at[ch, idx(s)], rss.at[ch, s], rrs.at[ch, s], s)

    def swap_out(dst, g):
        def body(i, carry):
            for e in range(16):
                n = i * 16 + e
                dst[n, pl.ds(pl.multiple_of(g * 16, 16), 16), :] = (
                    tb[pl.ds(n, 16, stride=PB), :].astype(BF16))
            return carry
        lax.fori_loop(0, 8, body, 0)

    def chunk(ch, final):
        for s in range(1, ND):
            out_arrival(ch, s).wait_recv()
        loads = []
        for s in range(ND):
            src = recv.at[ch, idx(s)] if s else out_src(ch, 0)
            loads.append(pltpu.make_async_copy(
                src, p.at[cols_of(s), rows_of(s), :], psem.at[s]))
            loads[-1].start()
        for load in loads:
            load.wait()

        def one(g, carry):
            for e in range(8):
                j = g * 16 + 2 * e
                y = dot(a1[...], jnp.concatenate([p[j], p[j + 1]], axis=1))
                tb[2 * e * PB:2 * e * PB + 128, :] = y[:, :128]
                tb[(2 * e + 1) * PB:(2 * e + 1) * PB + 128, :] = y[:, 128:]
            swap_out(u1, g)
            return carry

        lax.fori_loop(0, 8, one, 0)

        def two(g, carry):
            for e in range(8):
                i = g * 16 + 2 * e
                y = dot(a2[...], jnp.concatenate([u1[i], u1[i + 1]], axis=1))
                y = y.astype(BF16).astype(F32)
                w = jnp.concatenate([dv[i], dv[i + 1]], axis=1) * y
                z = dot(b2[...], w.astype(BF16))
                tb[2 * e * PB:2 * e * PB + 128, :] = z[:, :128]
                tb[(2 * e + 1) * PB:(2 * e + 1) * PB + 128, :] = z[:, 128:]
            swap_out(v2, g)
            return carry

        lax.fori_loop(0, 8, two, 0)

        def three(g, carry):
            for e in range(4):
                j = g * 8 + 2 * e
                y = dot(b1[...], jnp.concatenate([v2[j], v2[j + 1]], axis=1)).astype(BF16)
                vo[j] = y[:, :128]
                vo[j + 1] = y[:, 128:]
            return carry

        lax.fori_loop(0, 16, three, 0)

        def vo_part(s, h):
            start = (col ^ (s >> 2)) * 64 + h * JA
            return vo.at[pl.ds(pl.multiple_of(start, 16), (JA, 64 - JA)[h]), rows_of(s), :]

        stores = []
        for s in range(0, ND):
            if final:
                part, h = s // 2 * 2, s % 2
                src, dst = vo_part(part, h), final[h][s // 2].at[core(0)]
            else:
                src = vo.at[cols_of(s), rows_of(s), :]
                dst = vs.at[ch, s] if s else q.at[ch, me]
            stores.append(pltpu.make_async_copy(src, dst, vsem.at[s]))
            stores[-1].start()
        if final:
            trades = [
                (remote(vo_part(s, h), final[h][s // 2].at[core(0)],
                        gss.at[s // 2, h], grs.at[s // 2, h], 1),
                 remote(vo_part(s, h), final[h][s // 2].at[core(1)],
                        gss.at[s // 2, h], grs.at[s // 2, h], 1))
                for s in range(1, ND, 2) for h in range(2)]
            for give, _ in trades:
                give.start()
            for give, take in trades:
                give.wait_send()
                take.wait_recv()
        for store in stores:
            store.wait()
        if not final:
            for s in ORDER:
                back_copy(ch, s).start()

    def early(ch, carry):
        chunk(ch, None)
        return carry

    lax.fori_loop(0, NE, early, 0)
    chunk(NE, ((ga0, ga1, ga2, ga3), (gb0, gb1, gb2, gb3)))

    w_store.wait()
    for s in (2, 4, 6):
        d_out(s).wait_send()
    for s in (0, 2, 4, 6):
        d_relay(s).wait_send()

    def finish(ch, carry):
        for s in range(1, ND):
            out_copy(ch, s).wait_send()
            back_copy(ch, s).wait_send()
            back_arrival(ch, s).wait_recv()
        return carry

    lax.fori_loop(0, NE, finish, 0)
    for s in range(1, ND):
        out_copy(NE, s).wait_send()


def exchange(x, a3, a1, a2, b2, b1, b3, d):
    hbm = pl.BlockSpec(memory_space=pl.ANY)
    dma = pltpu.SemaphoreType.DMA
    piece = (64, 32, 128)
    return pl.pallas_call(
        exchange_kernel,
        out_shape=[
            jax.ShapeDtypeStruct((4, 4, 4) + piece, BF16),
            jax.ShapeDtypeStruct((ND, ND) + piece, BF16),
            jax.ShapeDtypeStruct((NE, ND) + piece, BF16),
            jax.ShapeDtypeStruct((NE, ND) + piece, BF16),
        ] + [jax.ShapeDtypeStruct((2, JA, 32, 128), BF16)] * 4 + [
        ] + [jax.ShapeDtypeStruct((2, 64 - JA, 32, 128), BF16)] * 4 + [
            jax.ShapeDtypeStruct((512, 512), BF16),
        ],
        in_specs=[hbm] * 8,
        out_specs=[hbm] * 13,
        scratch_shapes=[pltpu.VMEM((128, 128), BF16)] * 6 + [
            pltpu.VMEM((2, 32, JB, 16, 128), BF16),
            pltpu.VMEM((2, 4, 4, JB, 32, 128), BF16),
            pltpu.VMEM((32 * PA, 128), F32),
            pltpu.VMEM((JB * 128, 512), BF16),
            pltpu.VMEM((512, 512), BF16),
            pltpu.VMEM((512, 512), BF16),
            pltpu.VMEM((128, 128, 128), BF16),
            pltpu.VMEM((128, 128, 128), BF16),
            pltpu.VMEM((128, 128, 128), BF16),
            pltpu.VMEM((128, 128, 128), BF16),
            pltpu.VMEM((16 * PB, 128), F32),
            pltpu.VMEM((32, 64, 128), F32),
            pltpu.VMEM((4, 32, 16, 128), F32),
            pltpu.VMEM((ND, 32, 16, 128), F32),
            pltpu.VMEM((128, 128, 128), F32),
            dma((2,)), dma((2,)), dma((ND,)), dma((ND,)), dma(()), dma(()), dma((6,)),
            dma((ND,)), dma((ND,)),
            dma((ND, ND)), dma((ND, ND)), dma((NE, ND)), dma((NE, ND)), dma((4, 2)), dma((4, 2)),
        ],
        compiler_params=pltpu.CompilerParams(
            collective_id=0, has_side_effects=True, vmem_limit_bytes=56 * 1024 * 1024),
        name='exchange',
    )(x, a3, a1, a2, b2, b1, b3, d)[3:]


PC = 40


def early_kernel(q, wb, z, *ts):
    for j in range(JC):
        t = ts[j]
        parts = [q[:, c, :, j].reshape(NE * 2 * 32, 128) for c in range(4)]
        y = dot(jnp.concatenate(parts, axis=1), wb[...])
        for g in range(NE * 2):
            for r in range(4):
                k = (4 * g + r) * PC
                t[k:k + 32, :] = y[g * 32:(g + 1) * 32, r * 128:r * 128 + 128]
        for i in range(32):
            z[i, j] = t[pl.ds(i, NE * ND, stride=PC), :]


def early_last(q, wb):
    nr = NE * ND
    return pl.pallas_call(
        early_kernel,
        grid=(64 // JC,),
        out_shape=jax.ShapeDtypeStruct((32, 64, 64, 128), F32),
        in_specs=[
            pl.BlockSpec((NE, 4, 2, JC, 32, 128), lambda j: (0, 0, 0, j, 0, 0)),
            pl.BlockSpec((512, 512), lambda j: (0, 0)),
        ],
        out_specs=pl.BlockSpec((32, JC, nr, 128), lambda j: (0, j, 0, 0)),
        scratch_shapes=[pltpu.VMEM((nr * PC, 128), F32)] * JC,
        compiler_params=pltpu.CompilerParams(vmem_limit_bytes=40 * 1024 * 1024),
        cost_estimate=pl.CostEstimate(
            flops=2 * nr * 64 * 32 * 128 * 128, bytes_accessed=nr * 64 * 32 * 128 * 6, transcendentals=0),
        name='early_last',
    )(q.reshape(NE, 4, 2, 64, 32, 128), wb)


PF = JF * 32 + 8


def final_kernel(g0, g1, g2, g3, wb, z_in, z, *ts):
    row, col = lax.axis_index('row'), lax.axis_index('col')
    chip = col * 2 + lax.div(row, 2)
    n = JF * 32
    w = jnp.concatenate(
        [wb[pl.ds(pl.multiple_of((chip ^ c) * 128, 128), 128), :] for c in range(4)], axis=0)
    t = ts[0]
    for h in range(2):
        parts = [g[h].reshape(n, 128) for g in (g0, g1, g2, g3)]
        y = dot(jnp.concatenate(parts, axis=1), w)
        for r in range(4):
            k = (h * 4 + r) * PF
            t[k:k + n, :] = y[:, r * 128:r * 128 + 128]

    for j in range(JF):
        for i in range(32):
            z[i, j] = t[pl.ds(j * 32 + i, ND, stride=PF), :]


def final_last(pieces, wb, z, first, rows):
    return pl.pallas_call(
        final_kernel,
        grid=(rows // JF,),
        out_shape=jax.ShapeDtypeStruct((32, 64, 64, 128), F32),
        in_specs=[pl.BlockSpec((2, JF, 32, 128), lambda j: (0, j, 0, 0))] * 4 + [
            pl.BlockSpec((512, 512), lambda j: (0, 0)),
            pl.BlockSpec(memory_space=pl.ANY),
        ],
        out_specs=pl.BlockSpec((32, JF, ND, 128), lambda j: (0, j + first // JF, NE, 0)),
        scratch_shapes=[pltpu.VMEM((ND * PF, 128), F32)],
        input_output_aliases={5: 0},
        compiler_params=pltpu.CompilerParams(vmem_limit_bytes=40 * 1024 * 1024),
        cost_estimate=pl.CostEstimate(
            flops=2 * ND * rows * 32 * 128 * 128, bytes_accessed=ND * rows * 32 * 128 * 6, transcendentals=0),
        name='final_last',
    )(*pieces, wb, z)


def solution(mesh):
    vol_spec = P('row', 'col', None, 'rhs')
    diag_spec = P('row', 'col', None)
    full_spec = P(None, None)

    def local_op(volume, a_one, b_one, a_two, b_two, a_three, b_three, spectrum):
        x = jnp.transpose(volume, (0, 1, 3, 2))
        q, *pieces, wb = exchange(x, a_three, a_one, a_two, b_two, b_one, b_three, spectrum)
        parts = [pieces[:4], pieces[4:]]
        for part in parts:
            for c in (3, 2, 1):
                part[c] = lax.ppermute(part[c], ('col', 'row'), [(m, m ^ (2 * c)) for m in range(ND)])
        z = early_last(q, wb)
        z = final_last(parts[0], wb, z, 0, JA)
        z = final_last(parts[1], wb, z, JA, 64 - JA)
        return jnp.transpose(z, (0, 1, 3, 2))

    return jax.shard_map(
        local_op, mesh=mesh,
        in_specs=(vol_spec, full_spec, full_spec, full_spec, full_spec, full_spec, full_spec, diag_spec),
        out_specs=vol_spec, check_vma=False)
```

```python
import jax
import jax.numpy as jnp
from jax import lax
from jax.experimental import pallas as pl
from jax.experimental.pallas import tpu as pltpu
from jax.sharding import PartitionSpec as P

F32 = jnp.float32
BF16 = jnp.bfloat16
MESH = pl.DeviceIdType.MESH
LN = 128
VL = 56 << 20
VF = 40 << 20
ND = 8
ORDER = (6, 4, 2, 7, 5, 3, 1)
NE = ND - 1
JB = 4
PA = JB * 16 + 8
PB = 136
JC = 8
JA = 56
JF = 8


def dot(a, b):
    return jnp.dot(a, b, preferred_element_type=F32)


def exchange_kernel(x, a3_in, a1_in, a2_in, b2_in, b1_in, b3_in, d, u3, recv, vs, q,
                    ga0, ga1, ga2, ga3, gb0, gb1, gb2, gb3, wb,
                    a3, a1, a2, b2, b1, b3, xb, ub, ta, xs, w3, wv, p, u1, v2, vo, tb, dl, dp, dr, dv,
                    xsem, usem, psem, vsem, dsem, wsem, fsem, dss, drs, oss, ors, rss, rrs, gss, grs):
    row, col = lax.axis_index('row'), lax.axis_index('col')
    me = col * 4 + row

    def peer(s):
        return {'row': row ^ (s & 3), 'col': col ^ (s >> 2)}

    def idx(s):
        return (col ^ (s >> 2)) * 4 + (row ^ (s & 3))

    def chip(s):
        return lax.div(idx(s), 2)

    def core(s):
        return lax.rem(row ^ (s & 3), 2)

    def rows_of(s):
        return pl.ds(pl.multiple_of((row ^ (s & 3)) * 32, 32), 32)

    def cols_of(s):
        return pl.ds(pl.multiple_of((col ^ (s >> 2)) * 64, 64), 64)

    def remote(src, dst, send, recv_, s):
        return pltpu.make_async_remote_copy(
            src_ref=src, dst_ref=dst, send_sem=send, recv_sem=recv_,
            device_id=peer(s), device_id_type=MESH)

    bar = pltpu.get_barrier_semaphore()
    for s in range(1, ND):
        pl.semaphore_signal(bar, inc=1, device_id=peer(s), device_id_type=MESH)

    own_d = pltpu.make_async_copy(d, dl, dsem)
    own_d.start()
    factors = [pltpu.make_async_copy(src, dst, fsem.at[n]) for n, (src, dst) in enumerate(
        ((a3_in, a3), (a1_in, a1), (a2_in, a2), (b2_in, b2), (b1_in, b1), (b3_in, b3)))]
    for factor in factors:
        factor.start()

    lane = lax.broadcasted_iota(jnp.int32, (16, LN), 1)
    own_d.wait()

    def pack(i, carry):
        parts = [dl[i, 16 * b:16 * b + 16, :] for b in range(4)]
        for c in range(4):
            out = parts[0] if c == 0 else pltpu.roll(parts[0], (LN - 32 * c) % LN, 1)
            for b in range(1, 4):
                sh = (32 * (b - c)) % LN
                v = pltpu.roll(parts[b], sh, 1) if sh else parts[b]
                out = jnp.where(lane >= 32 * b, v, out)
            dp[c, i] = out
        return carry

    lax.fori_loop(0, 32, pack, 0, unroll=4)

    pl.semaphore_wait(bar, ND - 1)

    def d_out(s):
        return remote(dp.at[chip(s)], dr.at[me], dss.at[s], drs.at[s], s)

    def d_in(s):
        return remote(dp.at[chip(s)], dr.at[idx(s)], dss.at[s], drs.at[s], s)

    for s in (6, 4, 2):
        d_out(s).start()

    for factor in factors:
        factor.wait()

    w3[...] = jnp.zeros_like(w3)
    for c in range(4):
        for r in range(4):
            w3[c * LN + r * 32:c * LN + r * 32 + 32, r * LN:r * LN + LN] = (
                a3[c * 32:c * 32 + 32, :])

    def x_load(c, t, slot):
        return pltpu.make_async_copy(
            x.at[:, pl.ds(t * JB, JB), pl.ds(pl.multiple_of(c * 16, 16), 16), :],
            xb.at[slot], xsem.at[slot])

    def u_store(c, t, slot):
        return pltpu.make_async_copy(
            ub.at[slot], u3.at[c, :, :, pl.ds(t * JB, JB), :, :], usem.at[slot])

    def out_src(ch, s):
        return u3.at[ch // 2, (ch % 2) * 2 + core(s), chip(s)]

    def out_copy(ch, s):
        return remote(out_src(ch, s), recv.at[ch, me], oss.at[ch, s], ors.at[ch, s], s)

    def send_slab(c, b):
        part = pl.ds(b * 16, 16)
        for h in range(2):
            for s in ORDER:
                ch = 2 * c + h
                remote(out_src(ch, s).at[part], recv.at[ch, me].at[part],
                       oss.at[ch, s], ors.at[ch, s], s).start()

    def out_arrival(ch, s):
        return remote(out_src(ch, s), recv.at[ch, idx(s)], oss.at[ch, s], ors.at[ch, s], s)

    nt = 64 // JB

    def group(c, carry):
        x_load(c, 0, 0).start()

        def block(t, carry):
            slot = lax.rem(t, 2)

            @pl.when(t + 1 < nt)
            def _():
                x_load(c, t + 1, 1 - slot).start()

            x_load(c, t, slot).wait()

            @pl.when(t >= 2)
            def _():
                u_store(c, t - 2, slot).wait()

            @pl.when(jnp.logical_and(lax.rem(t, 4) == 1, t > 4))
            def _():
                send_slab(c, lax.div(t, 4) - 1)

            n = JB * 16
            for i in range(32):
                ta[i * PA:i * PA + n, :] = xb[slot, i].reshape(n, LN).astype(F32)
            m = JB * 32
            for r in range(16):
                for j in range(JB):
                    xs[(r // 4) * m + j * 32:(r // 4) * m + j * 32 + 32, (r % 4) * LN:(r % 4) * LN + LN] = (
                        ta[pl.ds(j * 16 + r, 32, stride=PA), :].astype(BF16))
            y = lax.dot_general(xs[...], w3[...], (((1,), (1,)), ((), ())),
                                preferred_element_type=F32).astype(BF16)
            for g in range(4):
                for c4 in range(4):
                    ub[slot, g, c4] = y[g * m:(g + 1) * m, c4 * LN:c4 * LN + LN].reshape(JB, 32, LN)
            u_store(c, t, slot).start()
            return carry

        lax.fori_loop(0, nt, block, 0)
        u_store(c, nt - 2, (nt - 2) % 2).wait()
        u_store(c, nt - 1, (nt - 1) % 2).wait()
        send_slab(c, 3)
        return carry

    lax.fori_loop(0, 4, group, 0)

    wv[...] = jnp.zeros_like(wv)
    b3t = b3[...].astype(F32).T.astype(BF16)
    for c in range(4):
        for r in range(4):
            wv[c * LN + r * 32:c * LN + r * 32 + 32, r * LN:r * LN + LN] = (
                b3t[c * 32:c * 32 + 32, :])
    w_store = pltpu.make_async_copy(wv, wb, wsem)
    w_store.start()

    for s in (2, 4, 6):
        d_in(s).wait_recv()

    def d_src(s):
        return dr.at[idx(s)] if s else dp.at[chip(0)]

    def d_relay(s):
        return remote(d_src(s), dr.at[idx(s)], dss.at[s + 1], drs.at[s + 1], 1)

    def d_relayed(s):
        return remote(d_src(s), dr.at[idx(s + 1)], dss.at[s + 1], drs.at[s + 1], 1)

    for s in (0, 2, 4, 6):
        d_relay(s).start()
    for s in (0, 2, 4, 6):
        d_relayed(s).wait_recv()

    def unpack(i, carry):
        for s in range(ND):
            g = dr[idx(s), i] if s else dp[chip(0), i]
            base_i = (row ^ (s & 3)) * 32
            base_j = (col ^ (s >> 2)) * 64
            for b in range(4):
                pair = pltpu.roll(g, 32 if b % 2 == 0 else 96, 1)
                v = jnp.where(lax.div(lane, 32) == b, g, pair)
                v = jnp.where(lax.div(lane, 64) == b // 2, v, pltpu.roll(v, 64, 1))
                dv[base_i + i, pl.ds(pl.multiple_of(base_j + 16 * b, 16), 16), :] = v
        return carry

    lax.fori_loop(0, 32, unpack, 0)

    def back_copy(ch, s):
        return remote(vs.at[ch, s], q.at[ch, me], rss.at[ch, s], rrs.at[ch, s], s)

    def back_arrival(ch, s):
        return remote(vs.at[ch, s], q.at[ch, idx(s)], rss.at[ch, s], rrs.at[ch, s], s)

    def swap_out(dst, g):
        def body(i, carry):
            for e in range(16):
                n = i * 16 + e
                dst[n, pl.ds(pl.multiple_of(g * 16, 16), 16), :] = (
                    tb[pl.ds(n, 16, stride=PB), :].astype(BF16))
            return carry
        lax.fori_loop(0, 8, body, 0)

    def chunk(ch, final):
        for s in range(1, ND):
            out_arrival(ch, s).wait_recv()
        loads = []
        for s in range(ND):
            src = recv.at[ch, idx(s)] if s else out_src(ch, 0)
            loads.append(pltpu.make_async_copy(
                src, p.at[cols_of(s), rows_of(s), :], psem.at[s]))
            loads[-1].start()
        for load in loads:
            load.wait()

        def one(g, carry):
            for e in range(8):
                j = g * 16 + 2 * e
                y = dot(a1[...], jnp.concatenate([p[j], p[j + 1]], axis=1))
                tb[2 * e * PB:2 * e * PB + LN, :] = y[:, :LN]
                tb[(2 * e + 1) * PB:(2 * e + 1) * PB + LN, :] = y[:, LN:]
            swap_out(u1, g)
            return carry

        lax.fori_loop(0, 8, one, 0)

        def two(g, carry):
            for e in range(8):
                i = g * 16 + 2 * e
                y = dot(a2[...], jnp.concatenate([u1[i], u1[i + 1]], axis=1))
                y = y.astype(BF16).astype(F32)
                w = jnp.concatenate([dv[i], dv[i + 1]], axis=1) * y
                z = dot(b2[...], w.astype(BF16))
                tb[2 * e * PB:2 * e * PB + LN, :] = z[:, :LN]
                tb[(2 * e + 1) * PB:(2 * e + 1) * PB + LN, :] = z[:, LN:]
            swap_out(v2, g)
            return carry

        lax.fori_loop(0, 8, two, 0)

        def three(g, carry):
            for e in range(4):
                j = g * 8 + 2 * e
                y = dot(b1[...], jnp.concatenate([v2[j], v2[j + 1]], axis=1)).astype(BF16)
                vo[j] = y[:, :LN]
                vo[j + 1] = y[:, LN:]
            return carry

        lax.fori_loop(0, 16, three, 0)

        def vo_part(s, h):
            start = (col ^ (s >> 2)) * 64 + h * JA
            return vo.at[pl.ds(pl.multiple_of(start, 8), (JA, 64 - JA)[h]), rows_of(s), :]

        stores = []
        for s in range(0, ND):
            if final:
                part, h = s // 2 * 2, s % 2
                src, dst = vo_part(part, h), final[h][s // 2].at[core(0)]
            else:
                src = vo.at[cols_of(s), rows_of(s), :]
                dst = vs.at[ch, s] if s else q.at[ch, me]
            stores.append(pltpu.make_async_copy(src, dst, vsem.at[s]))
            stores[-1].start()
        if final:
            trades = [
                (remote(vo_part(s, h), final[h][s // 2].at[core(0)],
                        gss.at[s // 2, h], grs.at[s // 2, h], 1),
                 remote(vo_part(s, h), final[h][s // 2].at[core(1)],
                        gss.at[s // 2, h], grs.at[s // 2, h], 1))
                for s in range(1, ND, 2) for h in range(2)]
            for give, _ in trades:
                give.start()
            for give, take in trades:
                give.wait_send()
                take.wait_recv()
        for store in stores:
            store.wait()
        if not final:
            for s in ORDER:
                back_copy(ch, s).start()

    def early(ch, carry):
        chunk(ch, None)
        return carry

    lax.fori_loop(0, NE, early, 0)
    chunk(NE, ((ga0, ga1, ga2, ga3), (gb0, gb1, gb2, gb3)))

    w_store.wait()
    for s in (2, 4, 6):
        d_out(s).wait_send()
    for s in (0, 2, 4, 6):
        d_relay(s).wait_send()

    def finish(ch, carry):
        for s in range(1, ND):
            out_copy(ch, s).wait_send()
            back_copy(ch, s).wait_send()
            back_arrival(ch, s).wait_recv()
        return carry

    lax.fori_loop(0, NE, finish, 0)
    for s in range(1, ND):
        out_copy(NE, s).wait_send()


def exchange(x, a3, a1, a2, b2, b1, b3, d):
    hbm = pl.BlockSpec(memory_space=pl.ANY)
    dma = pltpu.SemaphoreType.DMA
    piece = (64, 32, LN)
    return pl.pallas_call(
        exchange_kernel,
        out_shape=[
            jax.ShapeDtypeStruct((4, 4, 4) + piece, BF16),
            jax.ShapeDtypeStruct((ND, ND) + piece, BF16),
            jax.ShapeDtypeStruct((NE, ND) + piece, BF16),
            jax.ShapeDtypeStruct((NE, ND) + piece, BF16),
        ] + [jax.ShapeDtypeStruct((2, JA, 32, LN), BF16)] * 4 + [
        ] + [jax.ShapeDtypeStruct((2, 64 - JA, 32, LN), BF16)] * 4 + [
            jax.ShapeDtypeStruct((512, 512), BF16),
        ],
        in_specs=[hbm] * 8,
        out_specs=[hbm] * 13,
        scratch_shapes=[pltpu.VMEM((LN, LN), BF16)] * 6 + [
            pltpu.VMEM((2, 32, JB, 16, LN), BF16),
            pltpu.VMEM((2, 4, 4, JB, 32, LN), BF16),
            pltpu.VMEM((32 * PA, LN), F32),
            pltpu.VMEM((JB * LN, 512), BF16),
            pltpu.VMEM((512, 512), BF16),
            pltpu.VMEM((512, 512), BF16),
            pltpu.VMEM((LN, LN, LN), BF16),
            pltpu.VMEM((LN, LN, LN), BF16),
            pltpu.VMEM((LN, LN, LN), BF16),
            pltpu.VMEM((LN, LN, LN), BF16),
            pltpu.VMEM((16 * PB, LN), F32),
            pltpu.VMEM((32, 64, LN), F32),
            pltpu.VMEM((4, 32, 16, LN), F32),
            pltpu.VMEM((ND, 32, 16, LN), F32),
            pltpu.VMEM((LN, LN, LN), F32),
            dma((2,)), dma((2,)), dma((ND,)), dma((ND,)), dma(()), dma(()), dma((6,)),
            dma((ND,)), dma((ND,)),
            dma((ND, ND)), dma((ND, ND)), dma((NE, ND)), dma((NE, ND)), dma((4, 2)), dma((4, 2)),
        ],
        compiler_params=pltpu.CompilerParams(
            collective_id=0, has_side_effects=True, vmem_limit_bytes=VL),
        name='exchange',
    )(x, a3, a1, a2, b2, b1, b3, d)[3:]


PC = 40


def early_kernel(q, wb, z, *ts):
    for j in range(JC):
        t = ts[j % len(ts)]
        parts = [q[:, c, :, j].reshape(NE * 2 * 32, LN) for c in range(4)]
        y = dot(jnp.concatenate(parts, axis=1), wb[...])
        for g in range(NE * 2):
            for r in range(4):
                k = (4 * g + r) * PC
                t[k:k + 32, :] = y[g * 32:(g + 1) * 32, r * LN:r * LN + LN]
        for i in range(32):
            z[i, j] = t[pl.ds(i, NE * ND, stride=PC), :]


def early_last(q, wb):
    nr = NE * ND
    return pl.pallas_call(
        early_kernel,
        grid=(64 // JC,),
        out_shape=jax.ShapeDtypeStruct((32, 64, 64, LN), F32),
        in_specs=[
            pl.BlockSpec((NE, 4, 2, JC, 32, LN), lambda j: (0, 0, 0, j, 0, 0)),
            pl.BlockSpec((512, 512), lambda j: (0, 0)),
        ],
        out_specs=pl.BlockSpec((32, JC, nr, LN), lambda j: (0, j, 0, 0)),
        scratch_shapes=[pltpu.VMEM((nr * PC, LN), F32)] * 4,
        compiler_params=pltpu.CompilerParams(vmem_limit_bytes=VF),
        cost_estimate=pl.CostEstimate(
            flops=2 * nr * 64 * 32 * LN * LN, bytes_accessed=nr * 64 * 32 * LN * 6, transcendentals=0),
        name='early_last',
    )(q.reshape(NE, 4, 2, 64, 32, LN), wb)


JH = JF // 2
PF = JH * 32 + 8


def final_kernel(g0, g1, g2, g3, wb, z_in, z, *ts):
    row, col = lax.axis_index('row'), lax.axis_index('col')
    chip = col * 2 + lax.div(row, 2)
    n = JH * 32
    w = jnp.concatenate(
        [wb[pl.ds(pl.multiple_of((chip ^ c) * LN, LN), LN), :] for c in range(4)], axis=0)
    for b, t in enumerate(ts):
        parts = [g[:, b * JH:(b + 1) * JH].reshape(2 * n, LN) for g in (g0, g1, g2, g3)]
        y = dot(jnp.concatenate(parts, axis=1), w)
        for h in range(2):
            for r in range(4):
                k = (h * 4 + r) * PF
                t[k:k + n, :] = y[h * n:(h + 1) * n, r * LN:r * LN + LN]
        for j in range(JH):
            for i in range(32):
                z[i, b * JH + j] = t[pl.ds(j * 32 + i, ND, stride=PF), :]


def final_last(pieces, wb, z, first, rows):
    return pl.pallas_call(
        final_kernel,
        grid=(rows // JF,),
        out_shape=jax.ShapeDtypeStruct((32, 64, 64, LN), F32),
        in_specs=[pl.BlockSpec((2, JF, 32, LN), lambda j: (0, j, 0, 0))] * 4 + [
            pl.BlockSpec((512, 512), lambda j: (0, 0)),
            pl.BlockSpec(memory_space=pl.ANY),
        ],
        out_specs=pl.BlockSpec((32, JF, ND, LN), lambda j: (0, j + first // JF, NE, 0)),
        scratch_shapes=[pltpu.VMEM((ND * PF, LN), F32)] * 2,
        input_output_aliases={5: 0},
        compiler_params=pltpu.CompilerParams(vmem_limit_bytes=VF),
        cost_estimate=pl.CostEstimate(
            flops=2 * ND * rows * 32 * LN * LN, bytes_accessed=ND * rows * 32 * LN * 6, transcendentals=0),
        name='final_last',
    )(*pieces, wb, z)


def solution(mesh):
    vol_spec = P('row', 'col', None, 'rhs')
    diag_spec = P('row', 'col', None)
    full_spec = P(None, None)

    def local_op(volume, a_one, b_one, a_two, b_two, a_three, b_three, spectrum):
        x = jnp.transpose(volume, (0, 1, 3, 2))
        q, *pieces, wb = exchange(x, a_three, a_one, a_two, b_two, b_one, b_three, spectrum)
        parts = [pieces[:4], pieces[4:]]
        for part in parts:
            for c in (3, 2, 1):
                part[c] = lax.ppermute(part[c], ('col', 'row'), [(m, m ^ (2 * c)) for m in range(ND)])
        z = early_last(q, wb)
        z = final_last(parts[0], wb, z, 0, JA)
        z = final_last(parts[1], wb, z, JA, 64 - JA)
        return jnp.transpose(z, (0, 1, 3, 2))

    return jax.shard_map(
        local_op, mesh=mesh,
        in_specs=(vol_spec, full_spec, full_spec, full_spec, full_spec, full_spec, full_spec, diag_spec),
        out_specs=vol_spec, check_vma=False)
```

```python
import jax
import jax.numpy as jnp
from jax import lax
from jax.experimental import pallas as pl
from jax.experimental.pallas import tpu as pltpu
from jax.sharding import PartitionSpec as P

F32 = jnp.float32
BF16 = jnp.bfloat16
MESH = pl.DeviceIdType.MESH
LN = 128
VL = 56 << 20
VF = 40 << 20
ND = 8
ORDER = (6, 4, 2, 7, 5, 3, 1)
NE = ND - 1
JB = 4
PA = JB * 16 + 8
PB = 136
JC = 8
JA = 56
JF = 8


def dot(a, b):
    return jnp.dot(a, b, preferred_element_type=F32)


def exchange_kernel(x, a3_in, a1_in, a2_in, b2_in, b1_in, b3_in, d, u3, recv, vs, q,
                    ga0, ga1, ga2, ga3, gb0, gb1, gb2, gb3, wb,
                    a3, a1, a2, b2, b1, b3, xb, ub, ta, xs, w3, wv, p, u1, v2, vo, tb, dl, dp, dr, dv,
                    xsem, usem, psem, vsem, dsem, wsem, fsem, dss, drs, oss, ors, rss, rrs, gss, grs):
    row, col = lax.axis_index('row'), lax.axis_index('col')
    me = col * 4 + row

    def peer(s):
        return {'row': row ^ (s & 3), 'col': col ^ (s >> 2)}

    def idx(s):
        return (col ^ (s >> 2)) * 4 + (row ^ (s & 3))

    def chip(s):
        return lax.div(idx(s), 2)

    def core(s):
        return lax.rem(row ^ (s & 3), 2)

    def rows_of(s):
        return pl.ds(pl.multiple_of((row ^ (s & 3)) * 32, 32), 32)

    def cols_of(s):
        return pl.ds(pl.multiple_of((col ^ (s >> 2)) * 64, 64), 64)

    def remote(src, dst, send, recv_, s):
        return pltpu.make_async_remote_copy(
            src_ref=src, dst_ref=dst, send_sem=send, recv_sem=recv_,
            device_id=peer(s), device_id_type=MESH)

    bar = pltpu.get_barrier_semaphore()
    for s in range(1, ND):
        pl.semaphore_signal(bar, inc=1, device_id=peer(s), device_id_type=MESH)

    own_d = pltpu.make_async_copy(d, dl, dsem)
    own_d.start()
    factors = [pltpu.make_async_copy(src, dst, fsem.at[n]) for n, (src, dst) in enumerate(
        ((a3_in, a3), (a1_in, a1), (a2_in, a2), (b2_in, b2), (b1_in, b1), (b3_in, b3)))]
    for factor in factors:
        factor.start()

    lane = lax.broadcasted_iota(jnp.int32, (16, LN), 1)
    own_d.wait()

    def pack(i, carry):
        parts = [dl[i, 16 * b:16 * b + 16, :] for b in range(4)]
        for c in range(4):
            out = parts[0] if c == 0 else pltpu.roll(parts[0], (LN - 32 * c) % LN, 1)
            for b in range(1, 4):
                sh = (32 * (b - c)) % LN
                v = pltpu.roll(parts[b], sh, 1) if sh else parts[b]
                out = jnp.where(lane >= 32 * b, v, out)
            dp[c, i] = out
        return carry

    lax.fori_loop(0, 32, pack, 0, unroll=4)

    pl.semaphore_wait(bar, ND - 1)

    def d_out(s):
        return remote(dp.at[chip(s)], dr.at[me], dss.at[s], drs.at[s], s)

    def d_in(s):
        return remote(dp.at[chip(s)], dr.at[idx(s)], dss.at[s], drs.at[s], s)

    for s in (6, 4, 2):
        d_out(s).start()

    for factor in factors:
        factor.wait()

    w3[...] = jnp.zeros_like(w3)
    for c in range(4):
        for r in range(4):
            w3[c * LN + r * 32:c * LN + r * 32 + 32, r * LN:r * LN + LN] = (
                a3[c * 32:c * 32 + 32, :])

    def x_load(c, t, slot):
        return pltpu.make_async_copy(
            x.at[:, pl.ds(t * JB, JB), pl.ds(pl.multiple_of(c * 16, 16), 16), :],
            xb.at[slot], xsem.at[slot])

    def u_store(c, t, slot):
        return pltpu.make_async_copy(
            ub.at[slot], u3.at[c, :, :, pl.ds(t * JB, JB), :, :], usem.at[slot])

    def out_src(ch, s):
        return u3.at[ch // 2, (ch % 2) * 2 + core(s), chip(s)]

    def out_copy(ch, s):
        return remote(out_src(ch, s), recv.at[ch, me], oss.at[ch, s], ors.at[ch, s], s)

    def send_slab(c, b):
        part = pl.ds(b * 16, 16)
        for h in range(2):
            for s in ORDER:
                ch = 2 * c + h
                remote(out_src(ch, s).at[part], recv.at[ch, me].at[part],
                       oss.at[ch, s], ors.at[ch, s], s).start()

    def out_arrival(ch, s):
        return remote(out_src(ch, s), recv.at[ch, idx(s)], oss.at[ch, s], ors.at[ch, s], s)

    nt = 64 // JB

    def group(c, carry):
        x_load(c, 0, 0).start()

        def block(t, carry):
            slot = lax.rem(t, 2)

            @pl.when(t + 1 < nt)
            def _():
                x_load(c, t + 1, 1 - slot).start()

            x_load(c, t, slot).wait()

            @pl.when(t >= 2)
            def _():
                u_store(c, t - 2, slot).wait()

            @pl.when(jnp.logical_and(lax.rem(t, 4) == 1, t > 4))
            def _():
                send_slab(c, lax.div(t, 4) - 1)

            n = JB * 16
            for i in range(32):
                ta[i * PA:i * PA + n, :] = xb[slot, i].reshape(n, LN).astype(F32)
            m = JB * 32
            for r in range(16):
                for j in range(JB):
                    xs[(r // 4) * m + j * 32:(r // 4) * m + j * 32 + 32, (r % 4) * LN:(r % 4) * LN + LN] = (
                        ta[pl.ds(j * 16 + r, 32, stride=PA), :].astype(BF16))
            y = lax.dot_general(xs[...], w3[...], (((1,), (1,)), ((), ())),
                                preferred_element_type=F32).astype(BF16)
            for g in range(4):
                for c4 in range(4):
                    ub[slot, g, c4] = y[g * m:(g + 1) * m, c4 * LN:c4 * LN + LN].reshape(JB, 32, LN)
            u_store(c, t, slot).start()
            return carry

        lax.fori_loop(0, nt, block, 0)
        u_store(c, nt - 2, (nt - 2) % 2).wait()
        u_store(c, nt - 1, (nt - 1) % 2).wait()
        send_slab(c, 3)
        return carry

    lax.fori_loop(0, 4, group, 0)

    wv[...] = jnp.zeros_like(wv)
    b3t = b3[...].astype(F32).T.astype(BF16)
    for c in range(4):
        for r in range(4):
            wv[c * LN + r * 32:c * LN + r * 32 + 32, r * LN:r * LN + LN] = (
                b3t[c * 32:c * 32 + 32, :])
    w_store = pltpu.make_async_copy(wv, wb, wsem)
    w_store.start()

    for s in (2, 4, 6):
        d_in(s).wait_recv()

    def d_src(s):
        return dr.at[idx(s)] if s else dp.at[chip(0)]

    def d_relay(s):
        return remote(d_src(s), dr.at[idx(s)], dss.at[s + 1], drs.at[s + 1], 1)

    def d_relayed(s):
        return remote(d_src(s), dr.at[idx(s + 1)], dss.at[s + 1], drs.at[s + 1], 1)

    for s in (0, 2, 4, 6):
        d_relay(s).start()
    for s in (0, 2, 4, 6):
        d_relayed(s).wait_recv()

    def unpack(i, carry):
        for s in range(ND):
            g = dr[idx(s), i] if s else dp[chip(0), i]
            base_i = (row ^ (s & 3)) * 32
            base_j = (col ^ (s >> 2)) * 64
            for b in range(4):
                pair = pltpu.roll(g, 32 if b % 2 == 0 else 96, 1)
                v = jnp.where(lax.div(lane, 32) == b, g, pair)
                v = jnp.where(lax.div(lane, 64) == b // 2, v, pltpu.roll(v, 64, 1))
                dv[base_i + i, pl.ds(pl.multiple_of(base_j + 16 * b, 16), 16), :] = v
        return carry

    lax.fori_loop(0, 32, unpack, 0)

    def back_copy(ch, s):
        return remote(vs.at[ch, s], q.at[ch, me], rss.at[ch, s], rrs.at[ch, s], s)

    def back_arrival(ch, s):
        return remote(vs.at[ch, s], q.at[ch, idx(s)], rss.at[ch, s], rrs.at[ch, s], s)

    def swap_out(dst, g):
        def body(i, carry):
            for e in range(16):
                n = i * 16 + e
                dst[n, pl.ds(pl.multiple_of(g * 16, 16), 16), :] = (
                    tb[pl.ds(n, 16, stride=PB), :].astype(BF16))
            return carry
        lax.fori_loop(0, 8, body, 0)

    def chunk(ch, final):
        for s in range(1, ND):
            out_arrival(ch, s).wait_recv()
        loads = []
        for s in range(ND):
            src = recv.at[ch, idx(s)] if s else out_src(ch, 0)
            loads.append(pltpu.make_async_copy(
                src, p.at[cols_of(s), rows_of(s), :], psem.at[s]))
            loads[-1].start()
        for load in loads:
            load.wait()

        def one(g, carry):
            for e in range(8):
                j = g * 16 + 2 * e
                y = dot(a1[...], jnp.concatenate([p[j], p[j + 1]], axis=1))
                tb[2 * e * PB:2 * e * PB + LN, :] = y[:, :LN]
                tb[(2 * e + 1) * PB:(2 * e + 1) * PB + LN, :] = y[:, LN:]
            swap_out(u1, g)
            return carry

        lax.fori_loop(0, 8, one, 0)

        def two(g, carry):
            for e in range(8):
                i = g * 16 + 2 * e
                y = dot(a2[...], jnp.concatenate([u1[i], u1[i + 1]], axis=1))
                y = y.astype(BF16).astype(F32)
                w = jnp.concatenate([dv[i], dv[i + 1]], axis=1) * y
                z = dot(b2[...], w.astype(BF16))
                tb[2 * e * PB:2 * e * PB + LN, :] = z[:, :LN]
                tb[(2 * e + 1) * PB:(2 * e + 1) * PB + LN, :] = z[:, LN:]
            swap_out(v2, g)
            return carry

        lax.fori_loop(0, 8, two, 0)

        def three(g, carry):
            for e in range(4):
                j = g * 8 + 2 * e
                y = dot(b1[...], jnp.concatenate([v2[j], v2[j + 1]], axis=1)).astype(BF16)
                vo[j] = y[:, :LN]
                vo[j + 1] = y[:, LN:]
            return carry

        lax.fori_loop(0, 16, three, 0)

        def vo_part(s, h):
            start = (col ^ (s >> 2)) * 64 + h * JA
            return vo.at[pl.ds(pl.multiple_of(start, 8), (JA, 64 - JA)[h]), rows_of(s), :]

        stores = []
        for s in range(0, ND):
            if final:
                part, h = s // 2 * 2, s % 2
                src, dst = vo_part(part, h), final[h][s // 2].at[core(0)]
            else:
                src = vo.at[cols_of(s), rows_of(s), :]
                dst = vs.at[ch, s] if s else q.at[ch, me]
            stores.append(pltpu.make_async_copy(src, dst, vsem.at[s]))
            stores[-1].start()
        if final:
            trades = [
                (remote(vo_part(s, h), final[h][s // 2].at[core(0)],
                        gss.at[s // 2, h], grs.at[s // 2, h], 1),
                 remote(vo_part(s, h), final[h][s // 2].at[core(1)],
                        gss.at[s // 2, h], grs.at[s // 2, h], 1))
                for s in range(1, ND, 2) for h in range(2)]
            for give, _ in trades:
                give.start()
            for give, take in trades:
                give.wait_send()
                take.wait_recv()
        for store in stores:
            store.wait()
        if not final:
            for s in ORDER:
                back_copy(ch, s).start()

    def early(ch, carry):
        chunk(ch, None)
        return carry

    lax.fori_loop(0, NE, early, 0)
    chunk(NE, ((ga0, ga1, ga2, ga3), (gb0, gb1, gb2, gb3)))

    w_store.wait()
    for s in (2, 4, 6):
        d_out(s).wait_send()
    for s in (0, 2, 4, 6):
        d_relay(s).wait_send()

    def finish(ch, carry):
        for s in range(1, ND):
            out_copy(ch, s).wait_send()
            back_copy(ch, s).wait_send()
            back_arrival(ch, s).wait_recv()
        return carry

    lax.fori_loop(0, NE, finish, 0)
    for s in range(1, ND):
        out_copy(NE, s).wait_send()


def exchange(x, a3, a1, a2, b2, b1, b3, d):
    hbm = pl.BlockSpec(memory_space=pl.ANY)
    dma = pltpu.SemaphoreType.DMA
    piece = (64, 32, LN)
    return pl.pallas_call(
        exchange_kernel,
        out_shape=[
            jax.ShapeDtypeStruct((4, 4, 4) + piece, BF16),
            jax.ShapeDtypeStruct((ND, ND) + piece, BF16),
            jax.ShapeDtypeStruct((NE, ND) + piece, BF16),
            jax.ShapeDtypeStruct((NE, ND) + piece, BF16),
        ] + [jax.ShapeDtypeStruct((2, JA, 32, LN), BF16)] * 4 + [
        ] + [jax.ShapeDtypeStruct((2, 64 - JA, 32, LN), BF16)] * 4 + [
            jax.ShapeDtypeStruct((512, 512), BF16),
        ],
        in_specs=[hbm] * 8,
        out_specs=[hbm] * 13,
        scratch_shapes=[pltpu.VMEM((LN, LN), BF16)] * 6 + [
            pltpu.VMEM((2, 32, JB, 16, LN), BF16),
            pltpu.VMEM((2, 4, 4, JB, 32, LN), BF16),
            pltpu.VMEM((32 * PA, LN), F32),
            pltpu.VMEM((JB * LN, 512), BF16),
            pltpu.VMEM((512, 512), BF16),
            pltpu.VMEM((512, 512), BF16),
            pltpu.VMEM((LN, LN, LN), BF16),
            pltpu.VMEM((LN, LN, LN), BF16),
            pltpu.VMEM((LN, LN, LN), BF16),
            pltpu.VMEM((LN, LN, LN), BF16),
            pltpu.VMEM((16 * PB, LN), F32),
            pltpu.VMEM((32, 64, LN), F32),
            pltpu.VMEM((4, 32, 16, LN), F32),
            pltpu.VMEM((ND, 32, 16, LN), F32),
            pltpu.VMEM((LN, LN, LN), F32),
            dma((2,)), dma((2,)), dma((ND,)), dma((ND,)), dma(()), dma(()), dma((6,)),
            dma((ND,)), dma((ND,)),
            dma((ND, ND)), dma((ND, ND)), dma((NE, ND)), dma((NE, ND)), dma((4, 2)), dma((4, 2)),
        ],
        compiler_params=pltpu.CompilerParams(
            collective_id=0, has_side_effects=True, vmem_limit_bytes=VL),
        name='exchange',
    )(x, a3, a1, a2, b2, b1, b3, d)[3:]


PC = 40


def early_kernel(q, wb, z, *ts):
    for j in range(JC):
        t = ts[j % len(ts)]
        parts = [q[:, c, :, j].reshape(NE * 2 * 32, LN) for c in range(4)]
        y = dot(jnp.concatenate(parts, axis=1), wb[...])
        for g in range(NE * 2):
            for r in range(4):
                k = (4 * g + r) * PC
                t[k:k + 32, :] = y[g * 32:(g + 1) * 32, r * LN:r * LN + LN]
        for i in range(32):
            z[i, j] = t[pl.ds(i, NE * ND, stride=PC), :]


def early_last(q, wb):
    nr = NE * ND
    return pl.pallas_call(
        early_kernel,
        grid=(64 // JC,),
        out_shape=jax.ShapeDtypeStruct((32, 64, 64, LN), F32),
        in_specs=[
            pl.BlockSpec((NE, 4, 2, JC, 32, LN), lambda j: (0, 0, 0, j, 0, 0)),
            pl.BlockSpec((512, 512), lambda j: (0, 0)),
        ],
        out_specs=pl.BlockSpec((32, JC, nr, LN), lambda j: (0, j, 0, 0)),
        scratch_shapes=[pltpu.VMEM((nr * PC, LN), F32)] * 4,
        compiler_params=pltpu.CompilerParams(vmem_limit_bytes=VF),
        cost_estimate=pl.CostEstimate(
            flops=2 * nr * 64 * 32 * LN * LN, bytes_accessed=nr * 64 * 32 * LN * 6, transcendentals=0),
        name='early_last',
    )(q.reshape(NE, 4, 2, 64, 32, LN), wb)


JH = JF // 2
PF = JH * 32 + 8


def final_kernel(g3, g2, g1, g0, wb, z_in, z, *ts):
    row, col = lax.axis_index('row'), lax.axis_index('col')
    chip = col * 2 + lax.div(row, 2)
    n = JH * 32
    w = jnp.concatenate(
        [wb[pl.ds(pl.multiple_of((chip ^ c) * LN, LN), LN), :] for c in range(4)], axis=0)
    for b, t in enumerate(ts):
        parts = [g[:, b * JH:(b + 1) * JH].reshape(2 * n, LN) for g in (g0, g1, g2, g3)]
        y = dot(jnp.concatenate(parts, axis=1), w)
        for h in range(2):
            for r in range(4):
                k = (h * 4 + r) * PF
                t[k:k + n, :] = y[h * n:(h + 1) * n, r * LN:r * LN + LN]
        for j in range(JH):
            for i in range(32):
                z[i, b * JH + j] = t[pl.ds(j * 32 + i, ND, stride=PF), :]


def final_last(pieces, wb, z, first, rows):
    return pl.pallas_call(
        final_kernel,
        grid=(rows // JF,),
        out_shape=jax.ShapeDtypeStruct((32, 64, 64, LN), F32),
        in_specs=[pl.BlockSpec((2, JF, 32, LN), lambda j: (0, j, 0, 0))] * 4 + [
            pl.BlockSpec((512, 512), lambda j: (0, 0)),
            pl.BlockSpec(memory_space=pl.ANY),
        ],
        out_specs=pl.BlockSpec((32, JF, ND, LN), lambda j: (0, j + first // JF, NE, 0)),
        scratch_shapes=[pltpu.VMEM((ND * PF, LN), F32)] * 2,
        input_output_aliases={5: 0},
        compiler_params=pltpu.CompilerParams(vmem_limit_bytes=VF),
        cost_estimate=pl.CostEstimate(
            flops=2 * ND * rows * 32 * LN * LN, bytes_accessed=ND * rows * 32 * LN * 6, transcendentals=0),
        name='final_last',
    )(*reversed(pieces), wb, z)


def solution(mesh):
    vol_spec = P('row', 'col', None, 'rhs')
    diag_spec = P('row', 'col', None)
    full_spec = P(None, None)

    def local_op(volume, a_one, b_one, a_two, b_two, a_three, b_three, spectrum):
        x = jnp.transpose(volume, (0, 1, 3, 2))
        q, *pieces, wb = exchange(x, a_three, a_one, a_two, b_two, b_one, b_three, spectrum)
        parts = [pieces[:4], pieces[4:]]
        for part in parts:
            for c in (3, 2, 1):
                part[c] = lax.ppermute(part[c], ('col', 'row'), [(m, m ^ (2 * c)) for m in range(ND)])
        z = early_last(q, wb)
        z = final_last(parts[0], wb, z, 0, JA)
        z = final_last(parts[1], wb, z, JA, 64 - JA)
        return jnp.transpose(z, (0, 1, 3, 2))

    return jax.shard_map(
        local_op, mesh=mesh,
        in_specs=(vol_spec, full_spec, full_spec, full_spec, full_spec, full_spec, full_spec, diag_spec),
        out_specs=vol_spec, check_vma=False)
```

```python
import jax
import jax.numpy as jnp
from jax import lax
from jax.experimental import pallas as pl
from jax.experimental.pallas import tpu as pltpu
from jax.sharding import PartitionSpec as P

F32 = jnp.float32
BF16 = jnp.bfloat16
MESH = pl.DeviceIdType.MESH
LN = 128
VL = 56 << 20
VF = 40 << 20
ND = 8
ORDER = (6, 4, 2, 7, 5, 3, 1)
NE = ND - 1
JB = 4
PA = JB * 16 + 8
PB = 136
JC = 8
JA = 48
JF = 8


def dot(a, b):
    return jnp.dot(a, b, preferred_element_type=F32)


def exchange_kernel(x, a3_in, a1_in, a2_in, b2_in, b1_in, b3_in, d, u3, recv, vs, q,
                    ga0, ga1, ga2, ga3, gb0, gb1, gb2, gb3, wb,
                    a3, a1, a2, b2, b1, b3, xb, ub, ta, xs, w3, wv, p, u1, v2, vo, tb, dl, dp, dr, dv,
                    xsem, usem, psem, vsem, dsem, wsem, fsem, dss, drs, oss, ors, rss, rrs, gss, grs):
    row, col = lax.axis_index('row'), lax.axis_index('col')
    me = col * 4 + row

    def peer(s):
        return {'row': row ^ (s & 3), 'col': col ^ (s >> 2)}

    def idx(s):
        return (col ^ (s >> 2)) * 4 + (row ^ (s & 3))

    def chip(s):
        return lax.div(idx(s), 2)

    def core(s):
        return lax.rem(row ^ (s & 3), 2)

    def rows_of(s):
        return pl.ds(pl.multiple_of((row ^ (s & 3)) * 32, 32), 32)

    def cols_of(s):
        return pl.ds(pl.multiple_of((col ^ (s >> 2)) * 64, 64), 64)

    def remote(src, dst, send, recv_, s):
        return pltpu.make_async_remote_copy(
            src_ref=src, dst_ref=dst, send_sem=send, recv_sem=recv_,
            device_id=peer(s), device_id_type=MESH)

    bar = pltpu.get_barrier_semaphore()
    for s in range(1, ND):
        pl.semaphore_signal(bar, inc=1, device_id=peer(s), device_id_type=MESH)

    own_d = pltpu.make_async_copy(d, dl, dsem)
    own_d.start()
    factors = [pltpu.make_async_copy(src, dst, fsem.at[n]) for n, (src, dst) in enumerate(
        ((a3_in, a3), (a1_in, a1), (a2_in, a2), (b2_in, b2), (b1_in, b1), (b3_in, b3)))]
    for factor in factors:
        factor.start()

    lane = lax.broadcasted_iota(jnp.int32, (16, LN), 1)
    own_d.wait()

    def pack(i, carry):
        parts = [dl[i, 16 * b:16 * b + 16, :] for b in range(4)]
        for c in range(4):
            out = parts[0] if c == 0 else pltpu.roll(parts[0], (LN - 32 * c) % LN, 1)
            for b in range(1, 4):
                sh = (32 * (b - c)) % LN
                v = pltpu.roll(parts[b], sh, 1) if sh else parts[b]
                out = jnp.where(lane >= 32 * b, v, out)
            dp[c, i] = out
        return carry

    lax.fori_loop(0, 32, pack, 0, unroll=4)

    pl.semaphore_wait(bar, ND - 1)

    def d_out(s):
        return remote(dp.at[chip(s)], dr.at[me], dss.at[s], drs.at[s], s)

    def d_in(s):
        return remote(dp.at[chip(s)], dr.at[idx(s)], dss.at[s], drs.at[s], s)

    for s in (6, 4, 2):
        d_out(s).start()

    for factor in factors:
        factor.wait()

    w3[...] = jnp.zeros_like(w3)
    for c in range(4):
        for r in range(4):
            w3[c * LN + r * 32:c * LN + r * 32 + 32, r * LN:r * LN + LN] = (
                a3[c * 32:c * 32 + 32, :])

    def x_load(c, t, slot):
        return pltpu.make_async_copy(
            x.at[:, pl.ds(t * JB, JB), pl.ds(pl.multiple_of(c * 16, 16), 16), :],
            xb.at[slot], xsem.at[slot])

    def u_store(c, t, slot):
        return pltpu.make_async_copy(
            ub.at[slot], u3.at[c, :, :, pl.ds(t * JB, JB), :, :], usem.at[slot])

    def out_src(ch, s):
        return u3.at[ch // 2, (ch % 2) * 2 + core(s), chip(s)]

    def out_copy(ch, s):
        return remote(out_src(ch, s), recv.at[ch, me], oss.at[ch, s], ors.at[ch, s], s)

    def send_slab(c, b):
        part = pl.ds(b * 16, 16)
        for h in range(2):
            for s in ORDER:
                ch = 2 * c + h
                remote(out_src(ch, s).at[part], recv.at[ch, me].at[part],
                       oss.at[ch, s], ors.at[ch, s], s).start()

    def out_arrival(ch, s):
        return remote(out_src(ch, s), recv.at[ch, idx(s)], oss.at[ch, s], ors.at[ch, s], s)

    nt = 64 // JB

    def group(c, carry):
        x_load(c, 0, 0).start()

        def block(t, carry):
            slot = lax.rem(t, 2)

            @pl.when(t + 1 < nt)
            def _():
                x_load(c, t + 1, 1 - slot).start()

            x_load(c, t, slot).wait()

            @pl.when(t >= 2)
            def _():
                u_store(c, t - 2, slot).wait()

            @pl.when(jnp.logical_and(lax.rem(t, 4) == 1, t > 4))
            def _():
                send_slab(c, lax.div(t, 4) - 1)

            n = JB * 16
            for i in range(32):
                ta[i * PA:i * PA + n, :] = xb[slot, i].reshape(n, LN).astype(F32)
            m = JB * 32
            for r in range(16):
                for j in range(JB):
                    xs[(r // 4) * m + j * 32:(r // 4) * m + j * 32 + 32, (r % 4) * LN:(r % 4) * LN + LN] = (
                        ta[pl.ds(j * 16 + r, 32, stride=PA), :].astype(BF16))
            y = lax.dot_general(xs[...], w3[...], (((1,), (1,)), ((), ())),
                                preferred_element_type=F32).astype(BF16)
            for g in range(4):
                for c4 in range(4):
                    ub[slot, g, c4] = y[g * m:(g + 1) * m, c4 * LN:c4 * LN + LN].reshape(JB, 32, LN)
            u_store(c, t, slot).start()
            return carry

        lax.fori_loop(0, nt, block, 0)
        u_store(c, nt - 2, (nt - 2) % 2).wait()
        u_store(c, nt - 1, (nt - 1) % 2).wait()
        send_slab(c, 3)
        return carry

    lax.fori_loop(0, 4, group, 0)

    wv[...] = jnp.zeros_like(wv)
    b3t = b3[...].astype(F32).T.astype(BF16)
    for c in range(4):
        for r in range(4):
            wv[c * LN + r * 32:c * LN + r * 32 + 32, r * LN:r * LN + LN] = (
                b3t[c * 32:c * 32 + 32, :])
    w_store = pltpu.make_async_copy(wv, wb, wsem)
    w_store.start()

    for s in (2, 4, 6):
        d_in(s).wait_recv()

    def d_src(s):
        return dr.at[idx(s)] if s else dp.at[chip(0)]

    def d_relay(s):
        return remote(d_src(s), dr.at[idx(s)], dss.at[s + 1], drs.at[s + 1], 1)

    def d_relayed(s):
        return remote(d_src(s), dr.at[idx(s + 1)], dss.at[s + 1], drs.at[s + 1], 1)

    for s in (0, 2, 4, 6):
        d_relay(s).start()
    for s in (0, 2, 4, 6):
        d_relayed(s).wait_recv()

    def unpack(i, carry):
        for s in range(ND):
            g = dr[idx(s), i] if s else dp[chip(0), i]
            base_i = (row ^ (s & 3)) * 32
            base_j = (col ^ (s >> 2)) * 64
            for b in range(4):
                pair = pltpu.roll(g, 32 if b % 2 == 0 else 96, 1)
                v = jnp.where(lax.div(lane, 32) == b, g, pair)
                v = jnp.where(lax.div(lane, 64) == b // 2, v, pltpu.roll(v, 64, 1))
                dv[base_i + i, pl.ds(pl.multiple_of(base_j + 16 * b, 16), 16), :] = v
        return carry

    lax.fori_loop(0, 32, unpack, 0)

    def back_copy(ch, s):
        return remote(vs.at[ch, s], q.at[ch, me], rss.at[ch, s], rrs.at[ch, s], s)

    def back_arrival(ch, s):
        return remote(vs.at[ch, s], q.at[ch, idx(s)], rss.at[ch, s], rrs.at[ch, s], s)

    def swap_out(dst, g):
        def body(i, carry):
            for e in range(16):
                n = i * 16 + e
                dst[n, pl.ds(pl.multiple_of(g * 16, 16), 16), :] = (
                    tb[pl.ds(n, 16, stride=PB), :].astype(BF16))
            return carry
        lax.fori_loop(0, 8, body, 0)

    def chunk(ch, final):
        for s in range(1, ND):
            out_arrival(ch, s).wait_recv()
        loads = []
        for s in range(ND):
            src = recv.at[ch, idx(s)] if s else out_src(ch, 0)
            loads.append(pltpu.make_async_copy(
                src, p.at[cols_of(s), rows_of(s), :], psem.at[s]))
            loads[-1].start()
        for load in loads:
            load.wait()

        def one(g, carry):
            for e in range(8):
                j = g * 16 + 2 * e
                y = dot(a1[...], jnp.concatenate([p[j], p[j + 1]], axis=1))
                tb[2 * e * PB:2 * e * PB + LN, :] = y[:, :LN]
                tb[(2 * e + 1) * PB:(2 * e + 1) * PB + LN, :] = y[:, LN:]
            swap_out(u1, g)
            return carry

        lax.fori_loop(0, 8, one, 0)

        def two(g, carry):
            for e in range(8):
                i = g * 16 + 2 * e
                y = dot(a2[...], jnp.concatenate([u1[i], u1[i + 1]], axis=1))
                y = y.astype(BF16).astype(F32)
                w = jnp.concatenate([dv[i], dv[i + 1]], axis=1) * y
                z = dot(b2[...], w.astype(BF16))
                tb[2 * e * PB:2 * e * PB + LN, :] = z[:, :LN]
                tb[(2 * e + 1) * PB:(2 * e + 1) * PB + LN, :] = z[:, LN:]
            swap_out(v2, g)
            return carry

        lax.fori_loop(0, 8, two, 0)

        def three(g, carry):
            for e in range(4):
                j = g * 8 + 2 * e
                y = dot(b1[...], jnp.concatenate([v2[j], v2[j + 1]], axis=1)).astype(BF16)
                vo[j] = y[:, :LN]
                vo[j + 1] = y[:, LN:]
            return carry

        lax.fori_loop(0, 16, three, 0)

        def vo_part(s, h):
            start = (col ^ (s >> 2)) * 64 + h * JA
            return vo.at[pl.ds(pl.multiple_of(start, 8), (JA, 64 - JA)[h]), rows_of(s), :]

        stores = []
        for s in range(0, ND):
            if final:
                part, h = s // 2 * 2, s % 2
                src, dst = vo_part(part, h), final[h][s // 2].at[core(0)]
            else:
                src = vo.at[cols_of(s), rows_of(s), :]
                dst = vs.at[ch, s] if s else q.at[ch, me]
            stores.append(pltpu.make_async_copy(src, dst, vsem.at[s]))
            stores[-1].start()
        if final:
            trades = [
                (remote(vo_part(s, h), final[h][s // 2].at[core(0)],
                        gss.at[s // 2, h], grs.at[s // 2, h], 1),
                 remote(vo_part(s, h), final[h][s // 2].at[core(1)],
                        gss.at[s // 2, h], grs.at[s // 2, h], 1))
                for s in range(1, ND, 2) for h in range(2)]
            for give, _ in trades:
                give.start()
            for give, take in trades:
                give.wait_send()
                take.wait_recv()
        for store in stores:
            store.wait()
        if not final:
            for s in ORDER:
                back_copy(ch, s).start()

    def early(ch, carry):
        chunk(ch, None)
        return carry

    lax.fori_loop(0, NE, early, 0)
    chunk(NE, ((ga0, ga1, ga2, ga3), (gb0, gb1, gb2, gb3)))

    w_store.wait()
    for s in (2, 4, 6):
        d_out(s).wait_send()
    for s in (0, 2, 4, 6):
        d_relay(s).wait_send()

    def finish(ch, carry):
        for s in range(1, ND):
            out_copy(ch, s).wait_send()
            back_copy(ch, s).wait_send()
            back_arrival(ch, s).wait_recv()
        return carry

    lax.fori_loop(0, NE, finish, 0)
    for s in range(1, ND):
        out_copy(NE, s).wait_send()


def exchange(x, a3, a1, a2, b2, b1, b3, d):
    hbm = pl.BlockSpec(memory_space=pl.ANY)
    dma = pltpu.SemaphoreType.DMA
    piece = (64, 32, LN)
    return pl.pallas_call(
        exchange_kernel,
        out_shape=[
            jax.ShapeDtypeStruct((4, 4, 4) + piece, BF16),
            jax.ShapeDtypeStruct((ND, ND) + piece, BF16),
            jax.ShapeDtypeStruct((NE, ND) + piece, BF16),
            jax.ShapeDtypeStruct((NE, ND) + piece, BF16),
        ] + [jax.ShapeDtypeStruct((2, JA, 32, LN), BF16)] * 4 + [
        ] + [jax.ShapeDtypeStruct((2, 64 - JA, 32, LN), BF16)] * 4 + [
            jax.ShapeDtypeStruct((512, 512), BF16),
        ],
        in_specs=[hbm] * 8,
        out_specs=[hbm] * 13,
        scratch_shapes=[pltpu.VMEM((LN, LN), BF16)] * 6 + [
            pltpu.VMEM((2, 32, JB, 16, LN), BF16),
            pltpu.VMEM((2, 4, 4, JB, 32, LN), BF16),
            pltpu.VMEM((32 * PA, LN), F32),
            pltpu.VMEM((JB * LN, 512), BF16),
            pltpu.VMEM((512, 512), BF16),
            pltpu.VMEM((512, 512), BF16),
            pltpu.VMEM((LN, LN, LN), BF16),
            pltpu.VMEM((LN, LN, LN), BF16),
            pltpu.VMEM((LN, LN, LN), BF16),
            pltpu.VMEM((LN, LN, LN), BF16),
            pltpu.VMEM((16 * PB, LN), F32),
            pltpu.VMEM((32, 64, LN), F32),
            pltpu.VMEM((4, 32, 16, LN), F32),
            pltpu.VMEM((ND, 32, 16, LN), F32),
            pltpu.VMEM((LN, LN, LN), F32),
            dma((2,)), dma((2,)), dma((ND,)), dma((ND,)), dma(()), dma(()), dma((6,)),
            dma((ND,)), dma((ND,)),
            dma((ND, ND)), dma((ND, ND)), dma((NE, ND)), dma((NE, ND)), dma((4, 2)), dma((4, 2)),
        ],
        compiler_params=pltpu.CompilerParams(
            collective_id=0, has_side_effects=True, vmem_limit_bytes=VL),
        name='exchange',
    )(x, a3, a1, a2, b2, b1, b3, d)[3:]


PC = 40


def early_kernel(q, wb, z, *ts):
    for j in range(JC):
        t = ts[j % len(ts)]
        parts = [q[:, c, :, j].reshape(NE * 2 * 32, LN) for c in range(4)]
        y = dot(jnp.concatenate(parts, axis=1), wb[...])
        for g in range(NE * 2):
            for r in range(4):
                k = (4 * g + r) * PC
                t[k:k + 32, :] = y[g * 32:(g + 1) * 32, r * LN:r * LN + LN]
        for i in range(32):
            z[i, j] = t[pl.ds(i, NE * ND, stride=PC), :]


def early_last(q, wb):
    nr = NE * ND
    return pl.pallas_call(
        early_kernel,
        grid=(64 // JC,),
        out_shape=jax.ShapeDtypeStruct((32, 64, 64, LN), F32),
        in_specs=[
            pl.BlockSpec((NE, 4, 2, JC, 32, LN), lambda j: (0, 0, 0, j, 0, 0)),
            pl.BlockSpec((512, 512), lambda j: (0, 0)),
        ],
        out_specs=pl.BlockSpec((32, JC, nr, LN), lambda j: (0, j, 0, 0)),
        scratch_shapes=[pltpu.VMEM((nr * PC, LN), F32)] * 4,
        compiler_params=pltpu.CompilerParams(vmem_limit_bytes=VF),
        cost_estimate=pl.CostEstimate(
            flops=2 * nr * 64 * 32 * LN * LN, bytes_accessed=nr * 64 * 32 * LN * 6, transcendentals=0),
        name='early_last',
    )(q.reshape(NE, 4, 2, 64, 32, LN), wb)


JH = JF // 2
PF = JH * 32 + 8


def final_kernel(g2, g3, g1, g0, wb, z_in, z, *ts):
    row, col = lax.axis_index('row'), lax.axis_index('col')
    chip = col * 2 + lax.div(row, 2)
    n = JH * 32
    w = jnp.concatenate(
        [wb[pl.ds(pl.multiple_of((chip ^ c) * LN, LN), LN), :] for c in range(4)], axis=0)
    for b, t in enumerate(ts):
        parts = [g[:, b * JH:(b + 1) * JH].reshape(2 * n, LN) for g in (g0, g1, g2, g3)]
        y = dot(jnp.concatenate(parts, axis=1), w)
        for h in range(2):
            for r in range(4):
                k = (h * 4 + r) * PF
                t[k:k + n, :] = y[h * n:(h + 1) * n, r * LN:r * LN + LN]
        for j in range(JH):
            for i in range(32):
                z[i, b * JH + j] = t[pl.ds(j * 32 + i, ND, stride=PF), :]


def final_last(pieces, wb, z, first, rows):
    return pl.pallas_call(
        final_kernel,
        grid=(rows // JF,),
        out_shape=jax.ShapeDtypeStruct((32, 64, 64, LN), F32),
        in_specs=[pl.BlockSpec((2, JF, 32, LN), lambda j: (0, j, 0, 0))] * 4 + [
            pl.BlockSpec((512, 512), lambda j: (0, 0)),
            pl.BlockSpec(memory_space=pl.ANY),
        ],
        out_specs=pl.BlockSpec((32, JF, ND, LN), lambda j: (0, j + first // JF, NE, 0)),
        scratch_shapes=[pltpu.VMEM((ND * PF, LN), F32)] * 2,
        input_output_aliases={5: 0},
        compiler_params=pltpu.CompilerParams(vmem_limit_bytes=VF),
        cost_estimate=pl.CostEstimate(
            flops=2 * ND * rows * 32 * LN * LN, bytes_accessed=ND * rows * 32 * LN * 6, transcendentals=0),
        name='final_last',
    )(*[pieces[c] for c in (2, 3, 1, 0)], wb, z)


def solution(mesh):
    vol_spec = P('row', 'col', None, 'rhs')
    diag_spec = P('row', 'col', None)
    full_spec = P(None, None)

    def local_op(volume, a_one, b_one, a_two, b_two, a_three, b_three, spectrum):
        x = jnp.transpose(volume, (0, 1, 3, 2))
        q, *pieces, wb = exchange(x, a_three, a_one, a_two, b_two, b_one, b_three, spectrum)
        parts = [pieces[:4], pieces[4:]]
        for part in parts:
            for c in (3, 2, 1):
                part[c] = lax.ppermute(part[c], ('col', 'row'), [(m, m ^ (2 * c)) for m in range(ND)])
        z = early_last(q, wb)
        z = final_last(parts[0], wb, z, 0, JA)
        z = final_last(parts[1], wb, z, JA, 64 - JA)
        return jnp.transpose(z, (0, 1, 3, 2))

    return jax.shard_map(
        local_op, mesh=mesh,
        in_specs=(vol_spec, full_spec, full_spec, full_spec, full_spec, full_spec, full_spec, diag_spec),
        out_specs=vol_spec, check_vma=False)
```
